8 devices in a mesh: model: 2 (over z, y), data: 4 (over x, core).
Axes of the slice: x: 2, y: 2, z: 1, core: 2. Of those that a mesh axis runs over, the one named last changes fastest.
Arguments:
- act_in: bfloat16 [32768, 1280], P('data')
- grad_out: bfloat16 [32768, 1280], P('data')
- w_up: bfloat16 [2, 1280, 5120], P(None, None, 'model')
- w_down: bfloat16 [2, 5120, 1280], P(None, 'model')
- master_up: float32 [2, 1280, 5120], P(None, 'data', 'model')
- master_down: float32 [2, 5120, 1280], P(None, ('model', 'data'))
- mom_up: float32 [2, 1280, 5120], P(None, 'data', 'model')
- mom_down: float32 [2, 5120, 1280], P(None, ('model', 'data'))
- var_up: float32 [2, 1280, 5120], P(None, 'data', 'model')
- var_down: float32 [2, 5120, 1280], P(None, ('model', 'data'))
- learn_rate: float32 [1], replicated
- clip_norm: float32 [1], replicated
Outputs:
- output 1: bfloat16 [2, 1280, 5120], P(None, None, 'model')
- output 2: bfloat16 [2, 5120, 1280], P(None, 'model')
- output 3: float32 [2, 1280, 5120], P(None, 'data', 'model')
- output 4: float32 [2, 5120, 1280], P(None, ('model', 'data'))
- output 5: float32 [2, 1280, 5120], P(None, 'data', 'model')
- output 6: float32 [2, 5120, 1280], P(None, ('model', 'data'))
- output 7: float32 [2, 1280, 5120], P(None, 'data', 'model')
- output 8: float32 [2, 5120, 1280], P(None, ('model', 'data'))
- output 9: float32 [1], replicated
All inputs are finite; a program needn't handle non-finite values.
Results may differ from the reference program's by a relative error of at most 0.00147533.
Values are sent between devices in bfloat16 or wider.
A program may use at most 1 GiB of HBM per device.

```python
import jax
import jax.numpy as jnp
from jax import lax

D = 1280
FF = 5120
TOKENS_DEV = 8192
DATA = 4
STEP = 10
ROWS = DATA * TOKENS_DEV

BETA_ONE = 0.9
BETA_TWO = 0.95
ADAM_EPS = 1e-8
NORM_EPS = 1e-6


def matmul(left_op, right_op):
    return jnp.dot(left_op, right_op, preferred_element_type=jnp.float32)


def gelu_fwd(z_low):
    return jax.nn.gelu(z_low.astype(jnp.float32)).astype(jnp.bfloat16)


def gelu_back(z_low, grad_low):
    _, back_fn = jax.vjp(jax.nn.gelu, z_low.astype(jnp.float32))
    return back_fn(grad_low.astype(jnp.float32))[0].astype(jnp.bfloat16)


def block_grads(x_blk, dy_blk, w_up, w_down):
    z_one = matmul(x_blk, w_up[0]).astype(jnp.bfloat16)
    act_one = gelu_fwd(z_one)
    hid_two = matmul(act_one, w_down[0]).astype(jnp.bfloat16)
    z_two = matmul(hid_two, w_up[1]).astype(jnp.bfloat16)
    act_two = gelu_fwd(z_two)
    grad_w4 = matmul(act_two.T, dy_blk)
    dact_two = matmul(dy_blk, w_down[1].T).astype(jnp.bfloat16)
    dz_two = gelu_back(z_two, dact_two)
    grad_w3 = matmul(hid_two.T, dz_two)
    dhid_two = matmul(dz_two, w_up[1].T).astype(jnp.bfloat16)
    grad_w2 = matmul(act_one.T, dhid_two)
    dact_one = matmul(dhid_two, w_down[0].T).astype(jnp.bfloat16)
    dz_one = gelu_back(z_one, dact_one)
    grad_w1 = matmul(x_blk.T, dz_one)
    return jnp.stack([grad_w1, grad_w3]), jnp.stack([grad_w2, grad_w4])


def adam_update(master_arr, mom_arr, var_arr, grad_arr, clip_scale, lr_val):
    scaled = clip_scale * grad_arr
    new_mom = BETA_ONE * mom_arr + (1.0 - BETA_ONE) * scaled
    new_var = BETA_TWO * var_arr + (1.0 - BETA_TWO) * scaled * scaled
    mom_hat = new_mom / (1.0 - BETA_ONE ** STEP)
    var_hat = new_var / (1.0 - BETA_TWO ** STEP)
    new_master = master_arr - lr_val * mom_hat / (jnp.sqrt(var_hat) + ADAM_EPS)
    return new_master, new_mom, new_var


def setup_inputs(seed: int = 0) -> dict:
    key_list = jax.random.split(jax.random.key(seed), 10)
    w_scale = D ** -0.5
    master_up = jax.random.normal(key_list[0], (2, D, FF), jnp.float32) * w_scale
    master_down = jax.random.normal(key_list[1], (2, FF, D), jnp.float32) * w_scale
    w_up = master_up.astype(jnp.bfloat16)
    w_down = master_down.astype(jnp.bfloat16)
    act_in = jax.random.normal(key_list[2], (ROWS, D), jnp.float32).astype(jnp.bfloat16)
    grad_out = jax.random.normal(key_list[3], (ROWS, D), jnp.float32).astype(jnp.bfloat16)
    est_up, est_down = block_grads(act_in[:TOKENS_DEV], grad_out[:TOKENS_DEV], w_up, w_down)
    sq_up = jnp.sum(est_up * est_up, axis=(1, 2)) / DATA
    sq_down = jnp.sum(est_down * est_down, axis=(1, 2)) / DATA
    est_norm = jnp.sqrt(jnp.sum(sq_up) + jnp.sum(sq_down))
    clip_frac = jax.random.uniform(key_list[4], (1,), jnp.float32, 0.3, 0.6)
    clip_norm = clip_frac * est_norm
    rms_up = clip_frac * jnp.sqrt(sq_up / (D * FF))
    rms_down = clip_frac * jnp.sqrt(sq_down / (D * FF))
    mom_up = jax.random.normal(key_list[5], (2, D, FF), jnp.float32) * rms_up[:, None, None]
    mom_down = jax.random.normal(key_list[6], (2, FF, D), jnp.float32) * rms_down[:, None, None]
    var_up = jax.random.uniform(key_list[7], (2, D, FF), jnp.float32, 0.25, 2.0) * (rms_up * rms_up)[:, None, None]
    var_down = jax.random.uniform(key_list[8], (2, FF, D), jnp.float32, 0.25, 2.0) * (rms_down * rms_down)[:, None, None]
    learn_rate = jax.random.uniform(key_list[9], (1,), jnp.float32, 0.1, 0.25) * w_scale
    return {"act_in": act_in, "grad_out": grad_out, "w_up": w_up, "w_down": w_down, "master_up": master_up, "master_down": master_down, "mom_up": mom_up, "mom_down": mom_down, "var_up": var_up, "var_down": var_down, "learn_rate": learn_rate, "clip_norm": clip_norm}


def reference(act_in, grad_out, w_up, w_down, master_up, master_down, mom_up, mom_down, var_up, var_down, learn_rate, clip_norm):
    x_blocks = act_in.reshape(DATA, TOKENS_DEV, D)
    dy_blocks = grad_out.reshape(DATA, TOKENS_DEV, D)

    def body_fn(carry_sum, block_pair):
        part_up, part_down = block_grads(block_pair[0], block_pair[1], w_up, w_down)
        return (carry_sum[0] + part_up, carry_sum[1] + part_down), None

    zero_sums = (jnp.zeros((2, D, FF), jnp.float32), jnp.zeros((2, FF, D), jnp.float32))
    grad_sums, _ = lax.scan(body_fn, zero_sums, (x_blocks, dy_blocks))
    grad_up = grad_sums[0] / DATA
    grad_down = grad_sums[1] / DATA
    sq_total = jnp.sum(grad_up * grad_up) + jnp.sum(grad_down * grad_down)
    norm_val = jnp.sqrt(sq_total)
    clip_scale = jnp.minimum(1.0, clip_norm[0] / (norm_val + NORM_EPS))
    lr_val = learn_rate[0]
    new_master_up, new_mom_up, new_var_up = adam_update(master_up, mom_up, var_up, grad_up, clip_scale, lr_val)
    new_master_down, new_mom_down, new_var_down = adam_update(master_down, mom_down, var_down, grad_down, clip_scale, lr_val)
    return (new_master_up.astype(jnp.bfloat16), new_master_down.astype(jnp.bfloat16), new_master_up, new_master_down, new_mom_up, new_mom_down, new_var_up, new_var_down, norm_val.reshape(1))
```

```python
import functools

import jax
import jax.numpy as jnp
from jax import lax
from jax.experimental import pallas as pl
from jax.experimental.pallas import tpu as pltpu
from jax.sharding import PartitionSpec as P

STEP = 10
BETA_ONE = 0.9
BETA_TWO = 0.95
ADAM_EPS = 1e-8
NORM_EPS = 1e-6
MESH = pl.DeviceIdType.MESH
F32 = jnp.float32
BF16 = jnp.bfloat16
GELU_ONE = 0.7978845608028654
GELU_TWO = GELU_ONE * 0.044715
IS_UP = (False, True, False, True)
PIECES = (("s", 0), ("s", 1), ("s", 2), ("m", 0), ("s", 3), ("m", 1), ("m", 2), ("m", 3))
SUBS = 2


def adam_update(master_arr, mom_arr, var_arr, grad_arr, clip_scale, lr_val):
    scaled = clip_scale * grad_arr
    new_mom = BETA_ONE * mom_arr + (1.0 - BETA_ONE) * scaled
    new_var = BETA_TWO * var_arr + (1.0 - BETA_TWO) * scaled * scaled
    mom_hat = new_mom / (1.0 - BETA_ONE ** STEP)
    var_hat = new_var / (1.0 - BETA_TWO ** STEP)
    new_master = master_arr - lr_val * mom_hat / (jnp.sqrt(var_hat) + ADAM_EPS)
    return new_master, new_mom, new_var


def gelu_half(z):
    return 0.5 + 0.5 * jnp.tanh(z * (GELU_ONE + GELU_TWO * (z * z)))


def gelu_slope(z):
    sig = gelu_half(z)
    wide = z * (2.0 * GELU_ONE + (6.0 * GELU_TWO) * (z * z))
    return sig * (1.0 + (1.0 - sig) * wide)


def dot_nn(a, b):
    return jnp.dot(a, b, preferred_element_type=F32)


def dot_nt(a, b):
    return lax.dot_general(a, b, (((1,), (1,)), ((), ())), preferred_element_type=F32)


def dot_tn(a, b):
    return lax.dot_general(a, b, (((0,), (0,)), ((), ())), preferred_element_type=F32)


def grad_kernel(
    rows, bm, nc,
    x, dy, wu, wd, zeros,
    gfin, gsib, nrm, wou, wod, z1, a1, z3, a3, q3, q1, hbuf, hpart, pss, psm, rc, rx, ry, x3,
    wb, ring, gacc, outs, res, gs, side, ss, nbuf,
    s_x, s_w, s_ring, s_out, s_gacc, s_ps, s_res, s_gs, s_side,
    w_snd, w_rcv, g_snd, g_rcv, f_snd, f_rcv, n_snd, n_rcv,
):
    yy = lax.axis_index("model")
    dd = lax.axis_index("data")
    xx = dd // 2
    cc = dd % 2
    me = yy * 4 + dd
    d_sib = 2 * xx + (1 - cc)
    d_far = 2 * (1 - xx) + cc
    d_diag = 2 * (1 - xx) + (1 - cc)
    sib, xnb, ynb = (yy, d_sib), (yy, d_far), (1 - yy, dd)
    dim = x.shape[1]
    half = dim // 2
    quart = dim // 4
    nr = rows // bm
    kr = rows // 2
    row0 = yy * rows
    chunks = [slice(n, n + nc) for n in range(0, dim, nc)]

    def aligned(v, m):
        return pl.multiple_of(v, m)

    def local(src, dst, sem):
        return pltpu.make_async_copy(src, dst, sem)

    def remote(src, dst, snd, rcv, dev):
        return pltpu.make_async_remote_copy(
            src_ref=src, dst_ref=dst, send_sem=snd, recv_sem=rcv, device_id=dev, device_id_type=MESH
        )

    barrier = pltpu.get_barrier_semaphore()
    for o in range(1, 8):
        tid = (me + o) % 8
        pl.semaphore_signal(barrier, inc=1, device_id=(tid // 4, tid % 4), device_id_type=MESH)
    pl.semaphore_wait(barrier, 7)

    mats = ((wu, wou, 0), (wd, wod, 0), (wu, wou, 1), (wd, wod, 1))

    def chunk(ref, m, q, sub):
        k = mats[m][2]
        size = ref.shape[1] // 4
        part = size // SUBS
        return ref.at[k, pl.ds(aligned(q * size + sub * part, part), part), :]

    def w_y(m, sub):
        return remote(chunk(mats[m][0], m, dd, sub), chunk(mats[m][1], m, dd, sub),
                      w_snd.at[m, sub, 0], w_rcv.at[m, sub, 0], ynb)

    def w_x(m, sub):
        c = chunk(mats[m][1], m, dd, sub)
        return remote(c, c, w_snd.at[m, sub, 1], w_rcv.at[m, sub, 1], xnb)

    def w_c(m, sub):
        c = chunk(mats[m][1], m, dd, sub)
        return remote(c, c, w_snd.at[m, sub, 2], w_rcv.at[m, sub, 2], sib)

    def w_f(m, sub):
        c = chunk(mats[m][1], m, d_far, sub)
        return remote(c, c, w_snd.at[m, sub, 3], w_rcv.at[m, sub, 3], sib)

    def w_from(m, sub, which):
        q = (dd, d_far, d_sib, d_diag)[which]
        c = chunk(mats[m][1], m, q, sub)
        return remote(c, c, w_snd.at[m, sub, which], w_rcv.at[m, sub, which], sib)

    def got_y(m, sub):
        def fn():
            w_from(m, sub, 0).wait_recv()
            w_x(m, sub).start()
            w_c(m, sub).start()
        return fn

    def got_x(m, sub):
        def fn():
            w_from(m, sub, 1).wait_recv()
            w_f(m, sub).start()
        return fn

    def got_rest(m):
        def fn():
            for sub in range(SUBS):
                w_from(m, sub, 2).wait_recv()
                w_from(m, sub, 3).wait_recv()
        return fn

    def w_copies(kind, hf, k, pair):
        out = []
        for b in range(2):
            if kind == "u":
                src = (wu, wou)[hf].at[k, :, pl.ds(b * dim, dim)]
            else:
                src = (wd, wod)[hf].at[k, pl.ds(b * dim, dim), :]
            out.append(local(src, wb.at[2 * pair + b], s_w.at[2 * pair + b]))
        return out

    def w_load(kind, hf, k, pair):
        def fn():
            for c in w_copies(kind, hf, k, pair):
                c.start()
        return fn

    def w_wait(kind, hf, k, pair):
        def fn():
            for c in w_copies(kind, hf, k, pair):
                c.wait()
        return fn

    def run_loop(n, body, hooks):
        def f(it, carry):
            for key in sorted(hooks):
                @pl.when(it == key)
                def _(key=key):
                    for fn in hooks[key]:
                        fn()
            body(it)
            return carry
        lax.fori_loop(0, n, f, 0)

    def rslice(r):
        return pl.ds(aligned(r * bm, bm), bm)

    def x_copy(r):
        return local(x.at[pl.ds(aligned(row0 + r * bm, bm), bm), :], res.at[rslice(r), :], s_x.at[r])

    def act_out(dst, it, half0, b, buf):
        hf = half0 + it // nr
        return local(outs.at[buf], dst.at[hf, rslice(it % nr), pl.ds(b * dim, dim)], s_out.at[buf])

    def z_stage(nh, half0, pair0, z_dst, a_dst, hooks, wait_x=False):
        def epi(slot, zi, n):
            zb = gacc[slot, :bm, n].astype(BF16)
            outs[zi, :, n] = zb
            zf = zb.astype(F32)
            outs[zi + 1, :, n] = (zf * gelu_half(zf)).astype(BF16)

        def put(it, b):
            return (act_out(z_dst, it, half0, b, 2 * b), act_out(a_dst, it, half0, b, 2 * b + 1))

        def body(it):
            r = it % nr
            base = 2 * (pair0 + it // nr)
            if wait_x:
                x_copy(r).wait()

            @pl.when(it >= 2)
            def _():
                for c in put(it - 2, 1):
                    c.wait()
            for n in chunks:
                gacc[0, :bm, n] = dot_nn(res[rslice(r), :], wb[base, :, n])
                epi(1, 2, n)

            @pl.when(it >= 1)
            def _():
                for c in put(it - 1, 1):
                    c.start()
                for c in put(it - 1, 0):
                    c.wait()
            for n in chunks:
                gacc[1, :bm, n] = dot_nn(res[rslice(r), :], wb[base + 1, :, n])
                epi(0, 0, n)
            for c in put(it, 0):
                c.start()

        total = nr * nh
        run_loop(total, body, hooks)
        for c in put(total - 2, 1):
            c.wait()
        for n in chunks:
            epi(1, 2, n)
        for c in put(total - 1, 1):
            c.start()
        for c in put(total - 1, 0) + put(total - 1, 1):
            c.wait()

    def k_tiles(src, hf, r):
        return [local(src.at[hf, rslice(r), pl.ds(b * dim, dim)], ring.at[(r % 2) * 2 + b], s_ring.at[(r % 2) * 2 + b])
                for b in range(2)]

    def k_first(src, hf):
        def fn():
            for c in k_tiles(src, hf, 0):
                c.start()
        return fn

    def k_stage(src, hf, pair, trans, last, store, hooks):
        def part(r):
            if last:
                return local(hpart.at[rslice(r), :], gacc.at[r % 2, pl.ds(0, bm), :], s_gacc.at[r % 2])
            return local(gacc.at[r % 2, pl.ds(0, bm), :], hpart.at[rslice(r), :], s_gacc.at[r % 2])

        def keep(r):
            return local(res.at[rslice(r), :], hbuf.at[rslice(r), :], s_out.at[r % 2])

        if last:
            part(0).start()

        def body(r):
            slot = r % 2

            @pl.when(r + 1 < nr)
            def _():
                for c in k_tiles(src, hf, r + 1):
                    c.start()
                if last:
                    part(r + 1).start()
            for c in k_tiles(src, hf, r):
                c.wait()
            if last:
                part(r).wait()
                if store:
                    @pl.when(r >= 2)
                    def _():
                        keep(r - 2).wait()
            else:
                @pl.when(r >= 2)
                def _():
                    part(r - 2).wait()
            for n in chunks:
                if trans:
                    val = dot_nt(ring[slot * 2], wb[2 * pair, n, :]) + dot_nt(ring[slot * 2 + 1], wb[2 * pair + 1, n, :])
                else:
                    val = dot_nn(ring[slot * 2], wb[2 * pair, :, n]) + dot_nn(ring[slot * 2 + 1], wb[2 * pair + 1, :, n])
                if last:
                    res[rslice(r), n] = (val + gacc[slot, :bm, n]).astype(BF16)
                else:
                    gacc[slot, :bm, n] = val
            if not last:
                part(r).start()
            elif store:
                keep(r).start()

        run_loop(nr, body, hooks)
        if not last:
            part(nr - 2).wait()
            part(nr - 1).wait()
        elif store:
            keep(nr - 2).wait()
            keep(nr - 1).wait()

    def q_tile(src, it, b):
        buf = 2 * b + it % 2
        return local(src.at[it // nr, rslice(it % nr), pl.ds(b * dim, dim)], ring.at[buf], s_ring.at[buf])

    def q_first(src):
        def fn():
            q_tile(src, 0, 0).start()
        return fn

    def q_stage(z_src, q_dst, hooks):
        total = 2 * nr

        def epi(slot, buf, tile, n):
            e = gacc[slot, :bm, n].astype(BF16).astype(F32)
            outs[buf, :, n] = (e * gelu_slope(ring[tile, :, n].astype(F32))).astype(BF16)

        def body(it):
            r = it % nr
            base = 2 * (it // nr)
            q_tile(z_src, it, 1).start()

            @pl.when(it + 1 < total)
            def _():
                q_tile(z_src, it + 1, 0).start()

            @pl.when(it >= 1)
            def _():
                q_tile(z_src, it - 1, 1).wait()

            @pl.when(it >= 2)
            def _():
                act_out(q_dst, it - 2, 0, 1, 2).wait()
            for n in chunks:
                gacc[0, :bm, n] = dot_nt(res[rslice(r), :], wb[base, n, :])
                epi(1, 2, 2 + (it + 1) % 2, n)

            @pl.when(it >= 1)
            def _():
                act_out(q_dst, it - 1, 0, 1, 2).start()
                act_out(q_dst, it - 1, 0, 0, 0).wait()
            q_tile(z_src, it, 0).wait()
            for n in chunks:
                gacc[1, :bm, n] = dot_nt(res[rslice(r), :], wb[base + 1, n, :])
                epi(0, 0, it % 2, n)
            act_out(q_dst, it, 0, 0, 0).start()

        run_loop(total, body, hooks)
        act_out(q_dst, total - 2, 0, 1, 2).wait()
        q_tile(z_src, total - 1, 1).wait()
        for n in chunks:
            epi(1, 2, 2 + (total - 1) % 2, n)
        act_out(q_dst, total - 1, 0, 1, 2).start()
        act_out(q_dst, total - 1, 0, 0, 0).wait()
        act_out(q_dst, total - 1, 0, 1, 2).wait()

    alpha, beta = pl.ds(0, quart), pl.ds(quart, quart)

    def c_msg(k, t):
        return remote(pss.at[k, t], rc.at[k, t], g_snd.at[k, t], g_rcv.at[k, t], sib)

    def x_msg(k, i):
        src = (psm.at[k, 0, alpha], psm.at[k, 1, alpha], x3.at[k, 0])[i]
        return remote(src, rx.at[k, i], g_snd.at[k, 4 + i], g_rcv.at[k, 4 + i], xnb)

    def y_msg(k, i):
        src = (psm.at[k, 0, beta], psm.at[k, 2, beta], x3.at[k, 1])[i]
        return remote(src, ry.at[k, i], g_snd.at[k, 7 + i], g_rcv.at[k, 7 + i], ynb)

    def piece_of(s):
        ge3 = (s + 5) // 8
        eq4 = ((4 - s % 4) // 4) * ((s + 7) // 8)
        mine = ge3 - eq4
        t = mine * (s - 3 - s // 5) + (1 - mine) * (s - s // 4)
        oth = 1 - t % 2
        xr = 1 - t // 2
        return mine, oth, xx + xr * (1 - 2 * xx), (1 - cc) + mine * (2 * cc - 1)

    def g_tile(k, src, u):
        _, oth, xp, cp = piece_of(u // 2)
        krow = pl.ds(aligned((u % 2) * kr, kr), kr)
        if IS_UP[k]:
            return local(src.at[oth, krow, pl.ds(aligned(cp * dim, dim), dim)], gs.at[u % 2], s_gs.at[u % 2])
        col = pl.ds(aligned(xp * dim + cp * half, half), half)
        return local(src.at[oth, krow, col], gs.at[u % 2, :, pl.ds(0, half)], s_gs.at[u % 2])

    def g_first(k, src):
        def fn():
            g_tile(k, src, 0).start()
        return fn

    def res_copy(kind, h):
        rs = pl.ds(h * kr, kr)
        if kind == "h":
            src = hbuf.at[rs, :]
        else:
            src = (x if kind == "x" else dy).at[pl.ds(aligned(row0 + h * kr, kr), kr), :]
        return local(src, res.at[rs, :], s_res.at[h])

    def res_load(kind, h):
        def fn():
            res_copy(kind, h).start()
        return fn

    def g_stage(k, src, res_kind, hooks):
        def init(s):
            kind, t = PIECES[s]
            return local(zeros if kind == "s" else rc.at[k, t], gacc.at[s % 2], s_gacc.at[s % 2])

        def save(s):
            kind, t = PIECES[s]
            return local(gacc.at[s % 2], (pss if kind == "s" else psm).at[k, t], s_ps)

        init(0).start()
        init(1).start()
        hooks = {key: list(val) for key, val in hooks.items()}

        def before(s):
            def fn():
                init(s).wait()
                if s >= 1:
                    save(s - 1).start()
            return fn

        def after(s):
            def fn():
                save(s - 1).wait()
                kind, t = PIECES[s - 1]
                if kind == "s":
                    c_msg(k, t).start()
                elif t == 0:
                    x_msg(k, 0).start()
                    y_msg(k, 0).start()
                elif t == 1:
                    x_msg(k, 1).start()
                elif t == 2:
                    y_msg(k, 1).start()
                if s + 1 < 8:
                    kind, t = PIECES[s + 1]
                    if kind == "m":
                        c_msg(k, t).wait_recv()
                    init(s + 1).start()
            return fn

        for s in range(8):
            hooks.setdefault(2 * s, []).append(before(s))
            if s >= 1:
                hooks.setdefault(2 * s + 1, []).append(after(s))
        if res_kind is not None:
            for h in range(2):
                hooks.setdefault(h, []).append(lambda h=h: res_copy(res_kind, h).wait())

        def body(u):
            @pl.when(u + 1 < 16)
            def _():
                g_tile(k, src, u + 1).start()
            g_tile(k, src, u).wait()
            slot = (u // 2) % 2
            krow = pl.ds(aligned((u % 2) * kr, kr), kr)
            if IS_UP[k]:
                _, _, xp, _ = piece_of(u // 2)
                gacc[slot] += dot_tn(res[krow, pl.ds(aligned(xp * half, half), half)], gs[u % 2])
            else:
                gacc[slot] += dot_tn(gs[u % 2, :, :half], res[krow, :])

        run_loop(16, body, hooks)
        save(7).start()
        save(7).wait()

    nq = quart // 8

    def side_add(dst, a, b):
        side[dst] = side[a] + side[b]

    def side_scale(dst, parts):
        def f(i, acc):
            rs = pl.ds(aligned(i * 8, 8), 8)
            v = side[parts[0], rs, :]
            for p in parts[1:]:
                v = v + side[p, rs, :]
            v = v * 0.25
            side[dst, rs, :] = v
            v = v * v
            for n in range(0, dim, 128):
                acc = acc + v[:, n:n + 128]
            return acc
        ss[...] = lax.fori_loop(0, nq, f, ss[...])

    def side_in(i, src):
        return local(src, side.at[i], s_side.at[i])

    def side_out(i, dst):
        return local(side.at[i], dst, s_side.at[i])

    def join_phases(k):
        ins = ((0, psm.at[k, 1, beta]), (1, ry.at[k, 0]), (2, psm.at[k, 2, alpha]), (3, rx.at[k, 0]))

        def pa():
            x_msg(k, 0).wait_recv()
            y_msg(k, 0).wait_recv()
            for i, s in ins:
                side_in(i, s).start()

        def pb():
            for i, s in ins:
                side_in(i, s).wait()
            side_add(0, 0, 1)
            side_add(2, 2, 3)
            side_out(0, x3.at[k, 0]).start()
            side_out(2, x3.at[k, 1]).start()

        def pc():
            side_out(0, x3.at[k, 0]).wait()
            side_out(2, x3.at[k, 1]).wait()
            x_msg(k, 2).start()
            y_msg(k, 2).start()
        return pa, pb, pc

    def to_sib(k):
        g = gfin.at[k, pl.ds(aligned((1 - cc) * quart, quart), quart), :]
        return remote(g, gsib.at[k // 2], f_snd.at[k // 2], f_rcv.at[k // 2], sib)

    def final_phases(k):
        ina = ((0, psm.at[k, 3, alpha]), (1, rx.at[k, 1]), (2, ry.at[k, 2]))
        inb = ((0, psm.at[k, 3, beta]), (1, ry.at[k, 1]), (2, rx.at[k, 2]))

        def pa():
            x_msg(k, 1).wait_recv()
            y_msg(k, 2).wait_recv()
            for i, s in ina:
                side_in(i, s).start()

        def pb():
            for i, s in ina:
                side_in(i, s).wait()
            side_scale(3, (0, 1, 2))
            side_out(3, gfin.at[k, alpha]).start()
            y_msg(k, 1).wait_recv()
            x_msg(k, 2).wait_recv()
            for i, s in inb:
                side_in(i, s).start()

        def pc():
            side_out(3, gfin.at[k, alpha]).wait()
            for i, s in inb:
                side_in(i, s).wait()
            side_scale(0, (0, 1, 2))
            side_out(0, gfin.at[k, beta]).start()

        def pd():
            side_out(0, gfin.at[k, beta]).wait()
            if IS_UP[k]:
                to_sib(k).start()
        return pa, pb, pc, pd

    def at(first, fns):
        return {first + i: [fn] for i, fn in enumerate(fns)}

    def merge(*tables):
        out = {}
        for table in tables:
            for key, fns in table.items():
                out.setdefault(key, []).extend(fns)
        return out

    ss[...] = jnp.zeros_like(ss)
    for m in range(2):
        for sub in range(SUBS):
            w_y(m, sub).start()
    w_load("u", 0, 0, 0)()
    for r in range(nr):
        x_copy(r).start()
    w_load("d", 0, 0, 1)()
    for m in range(2, 4):
        for sub in range(SUBS):
            w_y(m, sub).start()

    w_wait("u", 0, 0, 0)()
    z_stage(1, 0, 0, z1, a1, merge({5 * nr // 8: [got_y(0, 0)]}, {nr - 1: [k_first(a1, 0)]}), wait_x=True)
    w_wait("d", 0, 0, 1)()
    k_stage(a1, 0, 1, False, False, False, merge(
        {2 * nr // 8: [got_y(0, 1)]}, {3 * nr // 8: [got_x(0, 0)]}, {7 * nr // 8: [got_y(1, 0), got_x(0, 1)]}))
    got_rest(0)()
    w_load("u", 1, 0, 0)()
    w_wait("u", 1, 0, 0)()
    z_stage(1, 1, 0, z1, a1, merge(
        {4 * nr // 8: [got_y(1, 1), got_x(1, 0)]}, {7 * nr // 8: [got_y(2, 0)]}, {nr - 1: [k_first(a1, 1)]}))
    got_x(1, 1)()
    got_rest(1)()
    w_load("d", 1, 0, 1)()
    w_load("u", 0, 1, 0)()
    w_wait("d", 1, 0, 1)()
    k_stage(a1, 1, 1, False, True, True, merge(
        {4 * nr // 8: [got_y(2, 1), got_x(2, 0)]}, {7 * nr // 8: [got_y(3, 0)]}))
    w_wait("u", 0, 1, 0)()

    def w3_other():
        got_x(2, 1)()
        got_rest(2)()
        w_load("u", 1, 1, 1)()
    z_stage(2, 0, 0, z3, a3, merge(
        {nr - 2: [w3_other]}, {nr: [w_wait("u", 1, 1, 1)]}, {nr + 1: [got_y(3, 1), got_x(3, 0)]},
        {2 * nr - nr // 2: [res_load("dy", 0)]}, {2 * nr - 1: [g_first(0, a3)]}))
    res_load("dy", 1)()
    w_load("d", 0, 1, 0)()

    def w4_other():
        got_x(3, 1)()
        got_rest(3)()
        w_load("d", 1, 1, 1)()
    g_stage(0, a3, "dy", merge({4: [w4_other]}, {14: [q_first(z3)]}))
    w_wait("d", 0, 1, 0)()
    q_stage(z3, q3, merge(
        {nr: [w_wait("d", 1, 1, 1)]}, at(4, join_phases(0)),
        {2 * nr - nr // 2: [res_load("h", 0)]}, {2 * nr - 1: [g_first(1, q3)]}))
    res_load("h", 1)()
    w_load("u", 0, 1, 0)()
    w_load("u", 1, 1, 1)()
    g_stage(1, q3, "h", {14: [k_first(q3, 0)]})
    w_wait("u", 0, 1, 0)()
    k_stage(q3, 0, 0, True, False, False, merge(at(4, final_phases(0)), {nr - 1: []}))
    k_first(q3, 1)()
    w_wait("u", 1, 1, 1)()
    k_stage(q3, 1, 1, True, True, False, at(1, join_phases(1)))
    w_load("d", 0, 0, 0)()
    w_load("d", 1, 0, 1)()
    g_first(2, a1)()
    g_stage(2, a1, None, {14: [q_first(z1)]})
    w_wait("d", 0, 0, 0)()
    q_stage(z1, q1, merge(
        {nr: [w_wait("d", 1, 0, 1)]}, at(0, final_phases(1)), at(5, join_phases(2)),
        {2 * nr - nr // 2: [res_load("x", 0)]}, {2 * nr - 1: [g_first(3, q1)]}))
    res_load("x", 1)()
    g_stage(3, q1, "x", at(10, final_phases(2)))
    for fn in join_phases(3):
        fn()
    for fn in final_phases(3):
        fn()

    nbuf[me] = ss[...]

    def n_send(o):
        tid = (me + o) % 8
        return remote(ss, nbuf.at[me], n_snd.at[o], n_rcv.at[o], (tid // 4, tid % 4))

    def n_recv(o):
        return remote(ss, nbuf.at[(me + 8 - o) % 8], n_snd.at[o], n_rcv.at[o], sib)

    for o in range(1, 8):
        n_send(o).start()
    for o in range(1, 8):
        n_recv(o).wait_recv()
    acc = nbuf[0]
    for i in range(1, 8):
        acc = acc + nbuf[i]
    nrm[...] = acc

    for k in (1, 3):
        to_sib(k).wait_recv()
        to_sib(k).wait_send()
    for o in range(1, 8):
        n_send(o).wait_send()
    for m in range(4):
        for sub in range(SUBS):
            for c in (w_y(m, sub), w_x(m, sub), w_c(m, sub), w_f(m, sub)):
                c.wait_send()
    for k in range(4):
        for t in range(4):
            c_msg(k, t).wait_send()
        for i in range(3):
            x_msg(k, i).wait_send()
            y_msg(k, i).wait_send()


def gradients(act_in, grad_out, w_up, w_down):
    rows = act_in.shape[0] // 2
    dim = act_in.shape[1]
    wide = w_up.shape[2]
    half, quart = dim // 2, dim // 4
    bm = rows // 8
    hbm = pltpu.HBM
    S = jax.ShapeDtypeStruct
    act = S((2, rows, wide), BF16)
    outs = [
        S((4, half, dim), F32), S((2, quart, dim), F32), S((8, 128), F32),
        S(w_up.shape, BF16), S(w_down.shape, BF16), act, act, act, act, act, act,
        S((rows, dim), BF16), S((rows, dim), F32),
        S((4, 4, half, dim), F32), S((4, 4, half, dim), F32), S((4, 4, half, dim), F32),
        S((4, 3, quart, dim), F32), S((4, 3, quart, dim), F32), S((4, 2, quart, dim), F32),
    ]
    out_specs = [pl.BlockSpec(memory_space=hbm) for _ in outs]
    out_specs[2] = pl.BlockSpec(memory_space=pltpu.VMEM)
    dma = pltpu.SemaphoreType.DMA
    scratch = [
        pltpu.VMEM((4, dim, dim), BF16), pltpu.VMEM((4, bm, dim), BF16), pltpu.VMEM((2, half, dim), F32),
        pltpu.VMEM((4, bm, dim), BF16), pltpu.VMEM((rows, dim), BF16), pltpu.VMEM((2, rows // 2, dim), BF16),
        pltpu.VMEM((4, quart, dim), F32), pltpu.VMEM((8, 128), F32), pltpu.VMEM((8, 8, 128), F32),
        dma((8,)), dma((4,)), dma((4,)), dma((4,)), dma((2,)), dma, dma((2,)), dma((2,)), dma((4,)),
        dma((4, SUBS, 4)), dma((4, SUBS, 4)), dma((4, 10)), dma((4, 10)), dma((2,)), dma((2,)), dma((8,)), dma((8,)),
    ]
    flops = 20 * rows * dim * 2 * wide
    return pl.pallas_call(
        functools.partial(grad_kernel, rows, bm, min(256, dim)),
        out_shape=outs,
        in_specs=[pl.BlockSpec(memory_space=hbm)] * 5,
        out_specs=out_specs,
        scratch_shapes=scratch,
        compiler_params=pltpu.CompilerParams(
            collective_id=0, has_side_effects=True, vmem_limit_bytes=66_900_000
        ),
        cost_estimate=pl.CostEstimate(flops=flops, bytes_accessed=1_500_000_000, transcendentals=0),
        name="grads",
    )(act_in, grad_out, w_up, w_down, jnp.zeros((half, dim), F32))[:3]


def solution(mesh):
    spec_rows = P("data", None)
    spec_wup = P(None, None, "model")
    spec_wdown = P(None, "model", None)
    spec_sup = P(None, "data", "model")
    spec_sdown = P(None, ("model", "data"), None)
    spec_scalar = P(None)

    def local_step(act_in, grad_out, w_up, w_down, master_up, master_down, mom_up, mom_down, var_up, var_down, learn_rate, clip_norm):
        gfin, gsib, squares = gradients(act_in, grad_out, w_up, w_down)
        core = lax.axis_index("data") % 2
        quart = gsib.shape[1]

        def up_grad(k):
            own = lax.dynamic_slice_in_dim(gfin[k], core * quart, quart, 0)
            other = gsib[k // 2]
            return jnp.concatenate([jnp.where(core == 0, own, other), jnp.where(core == 0, other, own)], axis=1)

        grad_up = jnp.stack([up_grad(3), up_grad(1)])
        grad_down = jnp.stack([gfin[2], gfin[0]])
        norm_val = jnp.sqrt(jnp.sum(squares))
        clip_scale = jnp.minimum(1.0, clip_norm[0] / (norm_val + NORM_EPS))
        lr_val = learn_rate[0]
        new_master_down, new_mom_down, new_var_down = adam_update(master_down, mom_down, var_down, grad_down, clip_scale, lr_val)
        new_w_down = lax.all_gather(new_master_down.astype(BF16), "data", axis=1, tiled=True)
        new_master_up, new_mom_up, new_var_up = adam_update(master_up, mom_up, var_up, grad_up, clip_scale, lr_val)
        new_w_up = lax.all_gather(new_master_up.astype(BF16), "data", axis=1, tiled=True)
        return (new_w_up, new_w_down, new_master_up, new_master_down, new_mom_up, new_mom_down, new_var_up, new_var_down, norm_val.reshape(1))

    return jax.shard_map(local_step, mesh=mesh, in_specs=(spec_rows, spec_rows, spec_wup, spec_wdown, spec_sup, spec_sdown, spec_sup, spec_sdown, spec_sup, spec_sdown, spec_scalar, spec_scalar), out_specs=(spec_wup, spec_wdown, spec_sup, spec_sdown, spec_sup, spec_sdown, spec_sup, spec_sdown, spec_scalar), check_vma=False)
```

```python
import functools

import jax
import jax.numpy as jnp
from jax import lax
from jax.experimental import pallas as pl
from jax.experimental.pallas import tpu as pltpu
from jax.sharding import PartitionSpec as P


STEP = 10
BETA_ONE = 0.9
BETA_TWO = 0.95
ADAM_EPS = 1e-8
NORM_EPS = 1e-6
MESH = pl.DeviceIdType.MESH
F32 = jnp.float32
BF16 = jnp.bfloat16
GELU_ONE = 0.7978845608028654
GELU_TWO = GELU_ONE * 0.044715
IS_UP = (False, True, False, True)
LONG = (("s", 0), ("s", 1), ("m", 0), ("s", 2), ("m", 1), ("s", 3), ("m", 2), ("m", 3))
SHORT = (("s", 0), ("s", 1), ("m", 0), ("s", 2), ("m", 1), ("m", 2))
SUBS = 2


def gelu_half(z):
    return 0.5 + 0.5 * jnp.tanh(z * (GELU_ONE + GELU_TWO * (z * z)))


def gelu_slope(z):
    square = z * z
    t = jnp.tanh(z * (GELU_ONE + GELU_TWO * square))
    ramp = z * (0.5 * GELU_ONE + (1.5 * GELU_TWO) * square)
    return (1.0 + t) * (0.5 + (1.0 - t) * ramp)


def dot_nn(a, b):
    return jnp.dot(a, b, preferred_element_type=F32)


def dot_nt(a, b):
    return lax.dot_general(a, b, (((1,), (1,)), ((), ())), preferred_element_type=F32)


def dot_tn(a, b):
    return lax.dot_general(a, b, (((0,), (0,)), ((), ())), preferred_element_type=F32)


def grad_kernel(
    rows, bm, bz, nc,
    x, dy, wu, wd,
    gfin, gsib, nrm, wou, wod, z1, a1, z3, a3, q3, q1, hbuf, ebuf, hpart, psm, rc, rx, ry, x3,
    wb, ring, gacc, outs, res, gs, side, ss, nbuf,
    s_x, s_w, s_ring, s_out, s_gacc, s_ps, s_res, s_gs, s_side,
    w_snd, w_rcv, g_snd, g_rcv, f_snd, f_rcv, n_snd, n_rcv,
):
    yy = lax.axis_index("model")
    dd = lax.axis_index("data")
    xx = dd // 2
    cc = dd % 2
    me = yy * 4 + dd
    d_sib = 2 * xx + (1 - cc)
    d_far = 2 * (1 - xx) + cc
    d_diag = 2 * (1 - xx) + (1 - cc)
    sib, xnb, ynb = (yy, d_sib), (yy, d_far), (1 - yy, dd)
    dim = x.shape[1]
    half = dim // 2
    quart = dim // 4
    nr = rows // bm
    nz = rows // bz
    kr = rows // 2
    row0 = yy * rows
    chunks = [slice(n, n + nc) for n in range(0, dim, nc)]

    def aligned(v, m):
        return pl.multiple_of(v, m)

    def local(src, dst, sem):
        return pltpu.make_async_copy(src, dst, sem)

    def remote(src, dst, snd, rcv, dev):
        return pltpu.make_async_remote_copy(
            src_ref=src, dst_ref=dst, send_sem=snd, recv_sem=rcv, device_id=dev, device_id_type=MESH
        )

    def meet():
        barrier = pltpu.get_barrier_semaphore()
        for o in range(1, 8):
            tid = (me + o) % 8
            pl.semaphore_signal(barrier, inc=1, device_id=(tid // 4, tid % 4), device_id_type=MESH)
        pl.semaphore_wait(barrier, 7)

    mats = ((wu, wou, 0), (wd, wod, 0), (wu, wou, 1), (wd, wod, 1))

    def chunk(ref, m, q, sub):
        k = mats[m][2]
        size = ref.shape[1] // 4
        part = size // SUBS
        return ref.at[k, pl.ds(aligned(q * size + sub * part, part), part), :]

    def w_y(m, sub):
        return remote(chunk(mats[m][0], m, dd, sub), chunk(mats[m][1], m, dd, sub),
                      w_snd.at[m, sub, 0], w_rcv.at[m, sub, 0], ynb)

    def w_x(m, sub):
        c = chunk(mats[m][1], m, dd, sub)
        return remote(c, c, w_snd.at[m, sub, 1], w_rcv.at[m, sub, 1], xnb)

    def w_c(m, sub):
        c = chunk(mats[m][1], m, dd, sub)
        return remote(c, c, w_snd.at[m, sub, 2], w_rcv.at[m, sub, 2], sib)

    def w_f(m, sub):
        c = chunk(mats[m][1], m, d_far, sub)
        return remote(c, c, w_snd.at[m, sub, 3], w_rcv.at[m, sub, 3], sib)

    def w_from(m, sub, which):
        q = (dd, d_far, d_sib, d_diag)[which]
        c = chunk(mats[m][1], m, q, sub)
        return remote(c, c, w_snd.at[m, sub, which], w_rcv.at[m, sub, which], sib)

    def got_y(m, sub):
        def fn():
            w_from(m, sub, 0).wait_recv()
            w_x(m, sub).start()
            w_c(m, sub).start()

        return fn

    def got_x(m, sub):
        def fn():
            w_from(m, sub, 1).wait_recv()
            w_f(m, sub).start()

        return fn

    def got_rest(m):
        def fn():
            for sub in range(SUBS):
                w_from(m, sub, 2).wait_recv()
                w_from(m, sub, 3).wait_recv()

        return fn

    def w_copies(kind, hf, k, pair):
        out = []
        for b in range(2):
            if kind == "u":
                src = (wu, wou)[hf].at[k, :, pl.ds(b * dim, dim)]
            else:
                src = (wd, wod)[hf].at[k, pl.ds(b * dim, dim), :]
            out.append(local(src, wb.at[2 * pair + b], s_w.at[2 * pair + b]))
        return out

    def w_load(kind, hf, k, pair):
        def fn():
            for c in w_copies(kind, hf, k, pair):
                c.start()

        return fn

    def w_wait(kind, hf, k, pair):
        def fn():
            for c in w_copies(kind, hf, k, pair):
                c.wait()

        return fn

    def run_loop(n, body, hooks):
        def f(it, carry):
            for key in sorted(hooks):
                @pl.when(it == key)
                def _(key=key):
                    for fn in hooks[key]:
                        fn()
            body(it)
            return carry

        lax.fori_loop(0, n, f, 0)

    def rslice(r):
        return pl.ds(aligned(r * bm, bm), bm)

    def zslice(r):
        return pl.ds(aligned(r * bz, bz), bz)

    def x_copy(r):
        return local(x.at[pl.ds(aligned(row0 + r * bz, bz), bz), :], res.at[zslice(r), :], s_x.at[r])

    def act_out(dst, it, half0, b, buf):
        hf = half0 + it // nz
        return local(outs.at[buf], dst.at[hf, zslice(it % nz), pl.ds(b * dim, dim)], s_out.at[buf])

    def out_waits(it, put):
        for c in put(it, 0, it):
            c.wait()

        @pl.when(it >= 1)
        def _():
            for c in put(it - 1, 1, it):
                c.wait()

    def out_starts(it, put):
        for c in put(it, 0, it):
            c.start()

        @pl.when(it >= 1)
        def _():
            for c in put(it - 1, 1, it):
                c.start()

    def z_stage(nh, half0, pair0, z_dst, a_dst, hooks, wait_x=False, ending=()):
        def epi(slot, zi, n):
            zb = gacc[slot, :bz, n].astype(BF16)
            outs[zi, :, n] = zb
            zf = zb.astype(F32)
            outs[zi + 1, :, n] = (zf * gelu_half(zf)).astype(BF16)

        def put(it, b, when):
            buf = 4 * (when % 2) + 2 * b
            return (act_out(z_dst, it, half0, b, buf), act_out(a_dst, it, half0, b, buf + 1))

        def body(it):
            r = it % nz
            base = 2 * (pair0 + it // nz)
            buf = 4 * (it % 2)
            if wait_x:
                x_copy(r).wait()

            @pl.when(it >= 2)
            def _():
                out_waits(it - 2, put)

            for n in chunks:
                gacc[0, :bz, n] = dot_nn(res[zslice(r), :], wb[base, :, n])
                epi(1, buf + 2, n)
            for n in chunks:
                gacc[1, :bz, n] = dot_nn(res[zslice(r), :], wb[base + 1, :, n])
                epi(0, buf, n)
            out_starts(it, put)

        total = nz * nh
        run_loop(total, body, hooks)
        for fn in ending:
            fn()
        out_waits(total - 2, put)
        for n in chunks:
            epi(1, 4 * (total % 2) + 2, n)
        for c in put(total - 1, 1, total):
            c.start()
        out_waits(total - 1, put)
        for c in put(total - 1, 1, total):
            c.wait()

    def k_tiles(src, hf, r):
        return [local(src.at[hf, rslice(r), pl.ds(b * dim, dim)], ring.at[(r % 2) * 2 + b], s_ring.at[(r % 2) * 2 + b])
                for b in range(2)]

    def k_first(src, hf):
        def fn():
            for c in k_tiles(src, hf, 0):
                c.start()

        return fn

    def k_stage(src, hf, pair, trans, store, hooks):
        last = store is not None

        def part(r):
            if last:
                return local(hpart.at[rslice(r), :], gacc.at[r % 2, pl.ds(0, bm), :], s_gacc.at[r % 2])
            return local(gacc.at[r % 2, pl.ds(0, bm), :], hpart.at[rslice(r), :], s_gacc.at[r % 2])

        def keep(r):
            return local(res.at[rslice(r), :], store.at[rslice(r), :], s_out.at[r % 2])

        if last:
            part(0).start()

        def body(r):
            slot = r % 2

            @pl.when(r + 1 < nr)
            def _():
                for c in k_tiles(src, hf, r + 1):
                    c.start()
                if last:
                    part(r + 1).start()

            for c in k_tiles(src, hf, r):
                c.wait()
            if last:
                part(r).wait()

                @pl.when(r >= 2)
                def _():
                    keep(r - 2).wait()
            else:
                @pl.when(r >= 2)
                def _():
                    part(r - 2).wait()
            for n in chunks:
                if trans:
                    val = dot_nt(ring[slot * 2], wb[2 * pair, n, :]) + dot_nt(ring[slot * 2 + 1], wb[2 * pair + 1, n, :])
                else:
                    val = dot_nn(ring[slot * 2], wb[2 * pair, :, n]) + dot_nn(ring[slot * 2 + 1], wb[2 * pair + 1, :, n])
                if last:
                    res[rslice(r), n] = (val + gacc[slot, :bm, n]).astype(BF16)
                else:
                    gacc[slot, :bm, n] = val
            if not last:
                part(r).start()
            else:
                keep(r).start()

        run_loop(nr, body, hooks)
        if not last:
            part(nr - 2).wait()
            part(nr - 1).wait()
        else:
            keep(nr - 2).wait()
            keep(nr - 1).wait()

    def q_tile(src, it, b):
        buf = 2 * b + it % 2
        return local(src.at[it // nz, zslice(it % nz), pl.ds(b * dim, dim)], ring.at[buf, pl.ds(0, bz), :], s_ring.at[buf])

    def q_first(src):
        def fn():
            q_tile(src, 0, 0).start()

        return fn

    def q_stage(z_src, q_dst, hooks, ending=()):
        total = 2 * nz

        def epi(slot, buf, tile, n):
            e = gacc[slot, :bz, n].astype(BF16).astype(F32)
            outs[buf, :, n] = (e * gelu_slope(ring[tile, :bz, n].astype(F32))).astype(BF16)

        def put(it, b, when):
            return (act_out(q_dst, it, 0, b, 4 * (when % 2) + 2 * b),)

        def body(it):
            r = it % nz
            base = 2 * (it // nz)
            buf = 4 * (it % 2)
            q_tile(z_src, it, 1).start()

            @pl.when(it + 1 < total)
            def _():
                q_tile(z_src, it + 1, 0).start()

            @pl.when(it >= 1)
            def _():
                q_tile(z_src, it - 1, 1).wait()

            @pl.when(it >= 2)
            def _():
                out_waits(it - 2, put)

            q_tile(z_src, it, 0).wait()
            for n in chunks:
                gacc[0, :bz, n] = dot_nt(res[zslice(r), :], wb[base, n, :])
                epi(1, buf + 2, 2 + (it + 1) % 2, n)
            for n in chunks:
                gacc[1, :bz, n] = dot_nt(res[zslice(r), :], wb[base + 1, n, :])
                epi(0, buf, it % 2, n)
            out_starts(it, put)

        run_loop(total, body, hooks)
        for fn in ending:
            fn()
        out_waits(total - 2, put)
        q_tile(z_src, total - 1, 1).wait()
        for n in chunks:
            epi(1, 4 * (total % 2) + 2, 2 + (total - 1) % 2, n)
        for c in put(total - 1, 1, total):
            c.start()
        out_waits(total - 1, put)
        for c in put(total - 1, 1, total):
            c.wait()

    alpha, beta = pl.ds(0, quart), pl.ds(quart, quart)

    def c_msg(k, t):
        slot = (LONG if k == 3 else SHORT).index(("s", t)) % 2 if k == 3 or t < 3 else 0
        return remote(gacc.at[slot], rc.at[k, t], g_snd.at[k, t], g_rcv.at[k, t], sib)

    def x_msg(k, i):
        src = (psm.at[k, 0, alpha], psm.at[k, 1, alpha], x3.at[k, 0])[i]
        return remote(src, rx.at[k, i], g_snd.at[k, 4 + i], g_rcv.at[k, 4 + i], xnb)

    def y_msg(k, i):
        src = (psm.at[k, 0, beta], psm.at[k, 2, beta], x3.at[k, 1])[i]
        return remote(src, ry.at[k, i], g_snd.at[k, 7 + i], g_rcv.at[k, 7 + i], ynb)

    def piece_of(s, count):
        v = s + s // (count - 1)
        mine = (1 - v % 2) * ((v + 7) // 8)
        t = mine * (v // 2 - 1) + (1 - mine) * ((v + 1) // 2)
        oth = 1 - t % 2
        xr = 1 - t // 2
        return mine, oth, xx + xr * (1 - 2 * xx), (1 - cc) + mine * (2 * cc - 1)

    def tile_of(k, src, u, oth, xp, cp):
        krow = pl.ds(aligned((u % 2) * kr, kr), kr)
        if IS_UP[k]:
            return local(src.at[oth, krow, pl.ds(aligned(cp * dim, dim), dim)], gs.at[u % 2], s_gs.at[u % 2])
        col = pl.ds(aligned(xp * dim + cp * half, half), half)
        return local(src.at[oth, krow, col], gs.at[u % 2, :, pl.ds(0, half)], s_gs.at[u % 2])

    def g_tile(k, src, u):
        _, oth, xp, cp = piece_of(u // 2, 8 if k == 3 else 6)
        return tile_of(k, src, u, oth, xp, cp)

    def g_first(k, src):
        def fn():
            g_tile(k, src, 0).start()

        return fn

    def g_dot(k, u, xp, n):
        krow = pl.ds(aligned((u % 2) * kr, kr), kr)
        if IS_UP[k]:
            return dot_tn(res[krow, pl.ds(aligned(xp * half, half), half)], gs[u % 2, :, n])
        return dot_tn(gs[u % 2, :, :half], res[krow, n])

    def res_copy(kind, h):
        rs = pl.ds(h * kr, kr)
        if kind in ("h", "e"):
            src = (hbuf if kind == "h" else ebuf).at[rs, :]
        else:
            src = (x if kind == "x" else dy).at[pl.ds(aligned(row0 + h * kr, kr), kr), :]
        return local(src, res.at[rs, :], s_res.at[h])

    def res_load(kind, h):
        def fn():
            res_copy(kind, h).start()

        return fn

    def g_stage(k, src, res_kind, hooks):
        pieces = LONG if k == 3 else SHORT
        count = len(pieces)

        def save(s):
            return local(gacc.at[s % 2], psm.at[k, pieces[s][1]], s_ps)

        def theirs(t):
            return [local(rc.at[k, t, rs], side.at[i], s_side.at[i]) for i, rs in enumerate((alpha, beta))]

        def send(t):
            if t == 0:
                x_msg(k, 0).start()
                y_msg(k, 0).start()
            elif t == 1:
                x_msg(k, 1).start()
            elif t == 2:
                y_msg(k, 1).start()

        hooks = {key: list(val) for key, val in hooks.items()}

        def first(s):
            def fn():
                if s >= 2 and pieces[s - 2][0] == "s":
                    c_msg(k, pieces[s - 2][1]).wait_send()
                if s >= 1:
                    if pieces[s - 1][0] == "s":
                        c_msg(k, pieces[s - 1][1]).start()
                    else:
                        save(s - 1).start()
                if pieces[s][0] == "m":
                    c_msg(k, pieces[s][1]).wait_recv()
                    for c in theirs(pieces[s][1]):
                        c.start()

            return fn

        def second(s):
            def fn():
                if s >= 1 and pieces[s - 1][0] == "m":
                    save(s - 1).wait()
                    send(pieces[s - 1][1])
                if pieces[s][0] == "m":
                    for c in theirs(pieces[s][1]):
                        c.wait()

            return fn

        for s in range(count):
            hooks.setdefault(2 * s, []).append(first(s))
            hooks.setdefault(2 * s + 1, []).append(second(s))
        if res_kind is not None:
            for h in range(2):
                hooks.setdefault(h, []).append(lambda h=h: res_copy(res_kind, h).wait())

        def body(u):
            @pl.when(u + 1 < 2 * count)
            def _():
                g_tile(k, src, u + 1).start()

            g_tile(k, src, u).wait()
            mine, _, xp, _ = piece_of(u // 2, count)
            again = u % 2
            slot = (u // 2) % 2
            for n in chunks:
                val = g_dot(k, u, xp, n)
                for i, rs in enumerate((slice(0, quart), slice(quart, half))):
                    more = gacc[slot, rs, n] + jnp.where(mine == 1, side[i + 2 * (1 - mine * again), :, n], 0.0)
                    gacc[slot, rs, n] = val[rs, :] + jnp.where(again == 1, more, 0.0)

        run_loop(2 * count, body, hooks)
        save(count - 1).start()
        save(count - 1).wait()
        send(pieces[count - 1][1])

    def last_tile(k, src, u):
        return tile_of(k, src, u, 0, xx, (1 - cc) + (u // 2) * (2 * cc - 1))

    def last_first(k, src, res_kind):
        def fn():
            res_load(res_kind, 0)()
            last_tile(k, src, 0).start()

        return fn

    def last_pieces(k, src, res_kind, hooks):
        res_load(res_kind, 1)()
        hooks = {key: list(val) for key, val in hooks.items()}
        for h in range(2):
            hooks.setdefault(h, []).append(lambda h=h: res_copy(res_kind, h).wait())
        hooks.setdefault(2, []).append(lambda: c_msg(k, 3).start())

        def body(u):
            @pl.when(u + 1 < 4)
            def _():
                last_tile(k, src, u + 1).start()

            last_tile(k, src, u).wait()
            slot = u // 2
            for n in chunks:
                gacc[slot, :, n] = g_dot(k, u, xx, n) + jnp.where(u % 2 == 1, gacc[slot, :, n], 0.0)

        run_loop(4, body, hooks)

    def sum_phases(k):
        def p0():
            for i in (1, 2):
                x_msg(k, i).wait_recv()
                y_msg(k, i).wait_recv()
            side_in(0, rx.at[k, 1]).start()
            side_in(1, ry.at[k, 2]).start()

        def p1():
            c_msg(k, 3).wait_send()
            c_msg(k, 3).wait_recv()
            side_in(2, rc.at[k, 3, alpha]).start()
            side_in(3, rc.at[k, 3, beta]).start()

        def p2():
            side_in(0, rx.at[k, 1]).wait()
            side_in(1, ry.at[k, 2]).wait()
            side_in(2, rc.at[k, 3, alpha]).wait()
            side_scale(0, (0, 1, 2), 0)
            side_out(0, gfin.at[k, alpha]).start()
            side_in(1, ry.at[k, 1]).start()
            side_in(2, rx.at[k, 2]).start()

        def p3():
            side_in(1, ry.at[k, 1]).wait()
            side_in(2, rx.at[k, 2]).wait()
            side_in(3, rc.at[k, 3, beta]).wait()
            side_scale(3, (1, 2, 3), quart)
            side_out(3, gfin.at[k, beta]).start()

        def p4():
            side_out(0, gfin.at[k, alpha]).wait()
            side_out(3, gfin.at[k, beta]).wait()
            if IS_UP[k]:
                to_sib(k).start()

        return p0, p1, p2, p3, p4

    nq = quart // 8

    def side_add(dst, a, b):
        side[dst] = side[a] + side[b]

    def side_scale(dst, parts, row=None):
        def f(i, acc):
            rs = pl.ds(aligned(i * 8, 8), 8)
            v = side[parts[0], rs, :]
            for p in parts[1:]:
                v = v + side[p, rs, :]
            if row is not None:
                v = v + gacc[1, pl.ds(aligned(row + i * 8, 8), 8), :]
            v = v * 0.25
            side[dst, rs, :] = v
            v = v * v
            for n in range(0, dim, 128):
                acc = acc + v[:, n:n + 128]
            return acc

        ss[...] = lax.fori_loop(0, nq, f, ss[...])

    def side_in(i, src):
        return local(src, side.at[i], s_side.at[i])

    def side_out(i, dst):
        return local(side.at[i], dst, s_side.at[i])

    def join_phases(k):
        ins = ((0, psm.at[k, 1, beta]), (1, ry.at[k, 0]), (2, psm.at[k, 2, alpha]), (3, rx.at[k, 0]))

        def pa():
            x_msg(k, 0).wait_recv()
            y_msg(k, 0).wait_recv()
            for i, s in ins:
                side_in(i, s).start()

        def pb():
            for i, s in ins:
                side_in(i, s).wait()
            side_add(0, 0, 1)
            side_add(2, 2, 3)
            side_out(0, x3.at[k, 0]).start()
            side_out(2, x3.at[k, 1]).start()

        def pc():
            side_out(0, x3.at[k, 0]).wait()
            side_out(2, x3.at[k, 1]).wait()
            x_msg(k, 2).start()
            y_msg(k, 2).start()

        return pa, pb, pc

    def to_sib(k):
        src = side.at[2 * (1 - cc)] if k == 3 else gfin.at[k, pl.ds(aligned((1 - cc) * quart, quart), quart), :]
        return remote(src, gsib.at[k // 2], f_snd.at[k // 2], f_rcv.at[k // 2], sib)

    def at(first, fns):
        return {first + i: [fn] for i, fn in enumerate(fns)}

    def merge(*tables):
        out = {}
        for table in tables:
            for key, fns in table.items():
                out.setdefault(key, []).extend(fns)
        return out

    w_load("u", 0, 0, 0)()
    for r in range(nz):
        x_copy(r).start()
    meet()
    for m in range(4):
        for sub in range(SUBS):
            w_y(m, sub).start()
    ss[...] = jnp.zeros_like(ss)

    w_wait("u", 0, 0, 0)()
    z_stage(1, 0, 0, z1, a1, merge(
        {4: [w_load("d", 0, 0, 1)]}, {10: [got_y(0, 0)]}, {15: [k_first(a1, 0)]}), wait_x=True)
    w_wait("d", 0, 0, 1)()
    k_stage(a1, 0, 1, False, None, merge(
        {1: [got_y(0, 1), got_x(0, 0)]}, {6: [got_y(1, 0), got_x(0, 1)]}, {7: [got_rest(0), w_load("u", 1, 0, 0)]}))
    w_wait("u", 1, 0, 0)()
    z_stage(1, 1, 0, z1, a1, merge(
        {4: [got_y(1, 1), got_x(1, 0)]},
        {12: [got_y(2, 0), got_x(1, 1), got_rest(1), w_load("d", 1, 0, 1)]}, {15: [k_first(a1, 1)]}))
    w_load("u", 0, 1, 0)()
    w_wait("d", 1, 0, 1)()
    k_stage(a1, 1, 1, False, hbuf, {3: [got_y(2, 1), got_x(2, 0)]})
    w_wait("u", 0, 1, 0)()
    z_stage(2, 0, 0, z3, a3, merge(
        {0: [got_y(3, 0), got_x(2, 1)]}, {9: [got_y(3, 1), got_x(3, 0)]},
        {11: [got_rest(2), w_load("u", 1, 1, 1)]}, {16: [w_wait("u", 1, 1, 1)]}, {20: [got_x(3, 1)]},
        {24: [res_load("dy", 0)]}, {31: [g_first(0, a3)]}), ending=(res_load("dy", 1),))
    g_stage(0, a3, "dy", merge(
        {3: [w_load("d", 0, 1, 0)]}, {5: [got_rest(3), w_load("d", 1, 1, 1)]}, {10: [q_first(z3)]}))
    w_wait("d", 0, 1, 0)()
    q_stage(z3, q3, merge(
        {16: [w_wait("d", 1, 1, 1)]}, at(8, join_phases(0)),
        {24: [res_load("h", 0)]}, {31: [g_first(1, q3)]}), ending=(res_load("h", 1),))
    g_stage(1, q3, "h", merge(
        {3: [w_load("u", 0, 1, 0)]}, {5: [w_load("u", 1, 1, 1)]}, {10: [k_first(q3, 0)]}))
    w_wait("u", 0, 1, 0)()
    k_stage(q3, 0, 0, True, None, at(5, join_phases(1)))
    k_first(q3, 1)()
    w_wait("u", 1, 1, 1)()
    k_stage(q3, 1, 1, True, ebuf, {nr - 1: [g_first(2, a1)]})
    g_stage(2, a1, None, merge(
        {3: [w_load("d", 0, 0, 0)]}, {5: [w_load("d", 1, 0, 1)]}, {10: [q_first(z1)]}))
    w_wait("d", 0, 0, 0)()
    q_stage(z1, q1, merge(
        {16: [w_wait("d", 1, 0, 1)]}, at(8, join_phases(2)),
        {24: [res_load("x", 0)]}, {31: [g_first(3, q1)]}), ending=(res_load("x", 1),))
    g_stage(3, q1, "x", {15: [last_first(0, a3, "dy")]})
    four, three, two = sum_phases(0), sum_phases(1), sum_phases(2)
    last_pieces(0, a3, "dy", {1: [four[0]], 3: [last_first(1, q3, "h")]})
    for fn in four[1:]:
        fn()
    for fn in join_phases(3):
        fn()
    last_pieces(1, q3, "h", {1: [three[0]], 3: [last_first(2, a1, "e")]})
    last_pieces(2, a1, "e", {0: [three[1]], 1: [three[2]], 2: [three[3]], 3: [three[4], two[0]]})
    for fn in two[1:]:
        fn()
    side_in(0, psm.at[3, 3, alpha]).start()
    side_in(2, psm.at[3, 3, beta]).start()
    x_msg(3, 1).wait_recv()
    side_in(1, rx.at[3, 1]).start()
    y_msg(3, 1).wait_recv()
    side_in(3, ry.at[3, 1]).start()
    side_in(0, psm.at[3, 3, alpha]).wait()
    side_in(1, rx.at[3, 1]).wait()
    side_add(0, 0, 1)
    side_in(2, psm.at[3, 3, beta]).wait()
    side_in(3, ry.at[3, 1]).wait()
    side_add(2, 2, 3)
    y_msg(3, 2).wait_recv()
    side_in(1, ry.at[3, 2]).start()
    x_msg(3, 2).wait_recv()
    side_in(3, rx.at[3, 2]).start()
    side_in(1, ry.at[3, 2]).wait()
    side_scale(0, (0, 1))
    side_out(0, gfin.at[3, alpha]).start()
    side_in(3, rx.at[3, 2]).wait()
    side_scale(2, (2, 3))
    side_out(2, gfin.at[3, beta]).start()
    to_sib(3).start()

    nbuf[me] = ss[...]

    def n_send(o):
        tid = (me + o) % 8
        return remote(ss, nbuf.at[me], n_snd.at[o], n_rcv.at[o], (tid // 4, tid % 4))

    def n_recv(o):
        return remote(ss, nbuf.at[(me + 8 - o) % 8], n_snd.at[o], n_rcv.at[o], sib)

    for o in range(1, 8):
        n_send(o).start()
    for o in range(1, 8):
        n_recv(o).wait_recv()
    acc = nbuf[0]
    for i in range(1, 8):
        acc = acc + nbuf[i]
    nrm[...] = acc

    side_out(0, gfin.at[3, alpha]).wait()
    side_out(2, gfin.at[3, beta]).wait()
    for k in (1, 3):
        to_sib(k).wait_recv()
        to_sib(k).wait_send()
    for o in range(1, 8):
        n_send(o).wait_send()
    for m in range(4):
        for sub in range(SUBS):
            for c in (w_y(m, sub), w_x(m, sub), w_c(m, sub), w_f(m, sub)):
                c.wait_send()
    for k in range(4):
        for i in range(3):
            x_msg(k, i).wait_send()
            y_msg(k, i).wait_send()


def gradients(act_in, grad_out, w_up, w_down):
    rows = act_in.shape[0] // 2
    dim = act_in.shape[1]
    wide = w_up.shape[2]
    half, quart = dim // 2, dim // 4
    bm, bz = rows // 8, rows // 16
    hbm = pltpu.HBM
    S = jax.ShapeDtypeStruct
    act = S((2, rows, wide), BF16)
    outs = [
        S((4, half, dim), F32), S((2, quart, dim), F32), S((8, 128), F32),
        S(w_up.shape, BF16), S(w_down.shape, BF16), act, act, act, act, act, act,
        S((rows, dim), BF16), S((rows, dim), BF16), S((rows, dim), F32),
        S((4, 4, half, dim), F32), S((4, 4, half, dim), F32),
        S((4, 3, quart, dim), F32), S((4, 3, quart, dim), F32), S((4, 2, quart, dim), F32),
    ]
    out_specs = [pl.BlockSpec(memory_space=hbm) for _ in outs]
    out_specs[2] = pl.BlockSpec(memory_space=pltpu.VMEM)
    dma = pltpu.SemaphoreType.DMA
    scratch = [
        pltpu.VMEM((4, dim, dim), BF16), pltpu.VMEM((4, bm, dim), BF16), pltpu.VMEM((2, half, dim), F32),
        pltpu.VMEM((8, bz, dim), BF16), pltpu.VMEM((rows, dim), BF16), pltpu.VMEM((2, rows // 2, dim), BF16),
        pltpu.VMEM((4, quart, dim), F32), pltpu.VMEM((8, 128), F32), pltpu.VMEM((8, 8, 128), F32),
        dma((16,)), dma((4,)), dma((4,)), dma((8,)), dma((2,)), dma, dma((2,)), dma((2,)), dma((4,)),
        dma((4, SUBS, 4)), dma((4, SUBS, 4)), dma((4, 10)), dma((4, 10)), dma((2,)), dma((2,)), dma((8,)), dma((8,)),
    ]
    flops = 20 * rows * dim * 2 * wide
    return pl.pallas_call(
        functools.partial(grad_kernel, rows, bm, bz, min(256, dim)),
        out_shape=outs,
        in_specs=[pl.BlockSpec(memory_space=hbm)] * 4,
        out_specs=out_specs,
        scratch_shapes=scratch,
        compiler_params=pltpu.CompilerParams(
            collective_id=0, has_side_effects=True, vmem_limit_bytes=66_900_000
        ),
        cost_estimate=pl.CostEstimate(flops=flops, bytes_accessed=1_500_000_000, transcendentals=0),
        name="grads",
    )(act_in, grad_out, w_up, w_down)[:3]


def update_kernel(is_up, where_ref, rate_ref, clip_ref, squares, *refs):
    grads, refs = refs[:1 + is_up], refs[1 + is_up:]
    master, mom, var = refs[:3]
    new_master, new_mom, new_var, wide, shard, scale = refs[-6:]
    cols = grads[0].shape[-1]

    @pl.when(pl.program_id(0) == 0)
    def _():
        norm = jnp.sqrt(jnp.sum(squares[...], keepdims=True))
        scale[...] = jnp.broadcast_to(jnp.minimum(1.0, clip_ref[0] / (norm + NORM_EPS)), scale.shape)

    clip_scale = scale[:1, :1]
    rate = rate_ref[0] / (1.0 - BETA_ONE ** STEP)
    for j in range(1 + is_up):
        cs = slice(j * cols, (j + 1) * cols)
        g = grads[0][0]
        if is_up:
            g = jnp.where(where_ref[1] == j, g, grads[1][0])
        scaled = clip_scale * g
        m = BETA_ONE * mom[0, :, cs] + (1.0 - BETA_ONE) * scaled
        v = BETA_TWO * var[0, :, cs] + ((1.0 - BETA_TWO) * scaled) * scaled
        new_mom[0, :, cs] = m
        new_var[0, :, cs] = v
        hat = v * (1.0 / (1.0 - BETA_TWO ** STEP))
        root = jnp.where(hat > 0.0, hat * lax.rsqrt(hat), 0.0)
        new = master[0, :, cs] - (rate * m) * pl.reciprocal(root + ADAM_EPS)
        new_master[0, :, cs] = new
        low = new.astype(BF16)
        wide[0, :, cs] = low
        shard[:, cs] = low


def update(is_up, k, mat, part, where, scalars, gfin, gsib, state, before):
    rows, cols = state[0].shape[1:]
    blocks = next(b for b in (5, 4, 2, 1) if rows % (32 * b) == 0)
    br = rows // (2 * blocks)
    skip = part * blocks
    dim = gfin.shape[2]

    def mine(i, w):
        return (mat, skip + i, 0)

    any_spec = pl.BlockSpec(memory_space=pl.ANY)
    state_spec = pl.BlockSpec((1, br, cols), mine)
    if is_up:
        g_specs = [pl.BlockSpec((1, br, dim), lambda i, w: (k, w[1] * 2 * blocks + skip + i, 0)), pl.BlockSpec((1, br, dim), lambda i, w: (k // 2, skip + i, 0))]
        g_args = [gfin, gsib]
    else:
        g_specs, g_args = [pl.BlockSpec((1, br, dim), lambda i, w: (k, skip + i, 0))], [gfin]
    held = list(before) if before is not None else []
    n_in = 4 + len(g_args) + 3
    smem = pl.BlockSpec(memory_space=pltpu.SMEM)
    S = jax.ShapeDtypeStruct
    shape = state[0].shape
    return pl.pallas_call(
        functools.partial(update_kernel, int(is_up)),
        out_shape=[S(shape, F32)] * 3 + [S((2, 4 * rows, cols), BF16), S((rows // 2, cols), BF16)],
        grid_spec=pltpu.PrefetchScalarGridSpec(
            num_scalar_prefetch=1, grid=(blocks,),
            in_specs=[smem, smem, pl.BlockSpec(memory_space=pltpu.VMEM)] + g_specs + [state_spec] * 3 + [any_spec] * len(held),
            out_specs=[state_spec] * 3 + [
                pl.BlockSpec((1, br, cols), lambda i, w: (mat, w[0] * 2 * blocks + skip + i, 0)), pl.BlockSpec((br, cols), lambda i, w: (i, 0))],
            scratch_shapes=[pltpu.VMEM((8, 128), F32)],
        ),
        input_output_aliases={n_in + i: i for i in range(len(held))},
        cost_estimate=pl.CostEstimate(flops=15 * rows * cols, bytes_accessed=16 * rows * cols, transcendentals=rows * cols),
        name="adam",
    )(where, *scalars, *g_args, *state, *held)


TO_FAR = [(0, 2), (2, 0), (1, 3), (3, 1)]
TO_SIB = [(0, 1), (1, 0), (2, 3), (3, 2)]


ORDER = [(up, k, mat, part) for up, k, mat in ((False, 2, 0), (False, 0, 1), (True, 3, 0), (True, 1, 1)) for part in (0, 1)]


def solution(mesh):
    spec_rows = P("data", None)
    spec_wup = P(None, None, "model")
    spec_wdown = P(None, "model", None)
    spec_sup = P(None, "data", "model")
    spec_sdown = P(None, ("model", "data"), None)
    spec_scalar = P(None)

    def local_step(act_in, grad_out, w_up, w_down, master_up, master_down, mom_up, mom_down, var_up, var_down, learn_rate, clip_norm):
        place = lax.axis_index("data")
        core = place % 2
        side = place // 2
        where = jnp.stack([place, core]).astype(jnp.int32)
        act_in, where = lax.optimization_barrier((act_in, where))
        gfin, gsib, squares = gradients(act_in, grad_out, w_up, w_down)
        norm_val = jnp.sqrt(jnp.sum(squares))
        scalars = (learn_rate, clip_norm, squares)
        state = {False: (master_down, mom_down, var_down), True: (master_up, mom_up, var_up)}
        done = {False: None, True: None}
        at_far, at_sib, at_diag = 2 * (1 - side) + core, 2 * side + 1 - core, 2 * (1 - side) + 1 - core

        def sib(shard):
            return lax.ppermute(shard, "data", TO_SIB)

        def put(is_up, mat, part, owner, piece):
            wide = done[is_up][3]
            start = owner * (wide.shape[1] // 4) + part * piece.shape[0]
            done[is_up][3] = lax.dynamic_update_slice(wide, piece[None], (mat, start, 0))

        sent = []
        for is_up, k, mat, part in ORDER:
            *done[is_up], shard = update(is_up, k, mat, part, where, scalars, gfin, gsib, state[is_up], done[is_up])
            where, shard = lax.optimization_barrier((where, shard))
            got = lax.ppermute(shard, "data", TO_FAR)
            sent.append((is_up, mat, part, shard, got))
        is_up, mat, part, shard, got = sent[0]
        put(is_up, mat, part, at_sib, sib(shard))
        late = None
        for i, (is_up, mat, part, shard, got) in enumerate(sent):
            got, done[True][3], done[False][3] = lax.optimization_barrier((got, done[True][3], done[False][3]))
            diag = sib(got)
            put(is_up, mat, part, at_far, got)
            if late is not None:
                put(*late)
            late = (is_up, mat, part, at_diag, diag)
            if i + 1 < len(sent):
                is_up, mat, part, shard, got = sent[i + 1]
                put(is_up, mat, part, at_sib, sib(shard))
        put(*late)
        up, down = done[True], done[False]
        new_w_up, new_w_down = up[3], down[3]
        return (new_w_up, new_w_down, up[0], down[0], up[1], down[1], up[2], down[2], norm_val.reshape(1))

    return jax.shard_map(local_step, mesh=mesh, in_specs=(spec_rows, spec_rows, spec_wup, spec_wdown, spec_sup, spec_sdown, spec_sup, spec_sdown, spec_sup, spec_sdown, spec_scalar, spec_scalar), out_specs=(spec_wup, spec_wdown, spec_sup, spec_sdown, spec_sup, spec_sdown, spec_sup, spec_sdown, spec_scalar), check_vma=False)
```

```python
import functools

import jax
import jax.numpy as jnp
from jax import lax
from jax.experimental import pallas as pl
from jax.experimental.pallas import tpu as pltpu
from jax.sharding import PartitionSpec as P


STEP = 10
BETA_ONE = 0.9
BETA_TWO = 0.95
ADAM_EPS = 1e-8
NORM_EPS = 1e-6
MESH = pl.DeviceIdType.MESH
F32 = jnp.float32
BF16 = jnp.bfloat16
GELU_ONE = 0.7978845608028654
GELU_TWO = GELU_ONE * 0.044715
IS_UP = (False, True, False, True)
SOON = (("s", 0), ("m", 0), ("s", 1), ("s", 2), ("m", 1), ("m", 2))
EVEN = (("s", 0), ("s", 1), ("m", 0), ("s", 2), ("m", 1), ("m", 2))
ORDERS = (EVEN, EVEN, EVEN, SOON)
SUBS = 2


def gelu_half(z):
    return 0.5 + 0.5 * jnp.tanh(z * (GELU_ONE + GELU_TWO * (z * z)))


def gelu_slope(z):
    square = z * z
    t = jnp.tanh(z * (GELU_ONE + GELU_TWO * square))
    ramp = z * (0.5 * GELU_ONE + (1.5 * GELU_TWO) * square)
    return (1.0 + t) * (0.5 + (1.0 - t) * ramp)


def dot_nn(a, b):
    return jnp.dot(a, b, preferred_element_type=F32)


def dot_nt(a, b):
    return lax.dot_general(a, b, (((1,), (1,)), ((), ())), preferred_element_type=F32)


def dot_tn(a, b):
    return lax.dot_general(a, b, (((0,), (0,)), ((), ())), preferred_element_type=F32)


def grad_kernel(
    rows, bm, bz, nc,
    x, dy, wu, wd,
    gfin, gsib, nrm, where, wou, wod, z1, a1, z3, a3, q3, q1, hbuf, ebuf, hpart, psm, rc, rx, ry, x3,
    wb, ring, gacc, outs, res, gs, side, ss, nbuf,
    s_x, s_w, s_ring, s_out, s_gacc, s_ps, s_res, s_gs, s_side,
    w_snd, w_rcv, g_snd, g_rcv, f_snd, f_rcv, n_snd, n_rcv,
):
    yy = lax.axis_index("model")
    dd = lax.axis_index("data")
    xx = dd // 2
    cc = dd % 2
    me = yy * 4 + dd
    d_sib = 2 * xx + (1 - cc)
    d_far = 2 * (1 - xx) + cc
    d_diag = 2 * (1 - xx) + (1 - cc)
    sib, xnb, ynb = (yy, d_sib), (yy, d_far), (1 - yy, dd)
    dim = x.shape[1]
    half = dim // 2
    quart = dim // 4
    nr = rows // bm
    nz = rows // bz
    kr = rows // 2
    row0 = yy * rows
    chunks = [slice(n, n + nc) for n in range(0, dim, nc)]

    def aligned(v, m):
        return pl.multiple_of(v, m)

    def local(src, dst, sem):
        return pltpu.make_async_copy(src, dst, sem)

    def remote(src, dst, snd, rcv, dev):
        return pltpu.make_async_remote_copy(
            src_ref=src, dst_ref=dst, send_sem=snd, recv_sem=rcv, device_id=dev, device_id_type=MESH
        )

    def meet():
        barrier = pltpu.get_barrier_semaphore()
        for o in range(1, 8):
            tid = (me + o) % 8
            pl.semaphore_signal(barrier, inc=1, device_id=(tid // 4, tid % 4), device_id_type=MESH)
        pl.semaphore_wait(barrier, 7)

    where[0] = dd
    where[1] = cc

    mats = ((wu, wou, 0), (wd, wod, 0), (wu, wou, 1), (wd, wod, 1))

    def chunk(ref, m, q, sub):
        k = mats[m][2]
        size = ref.shape[1] // 4
        part = size // SUBS
        return ref.at[k, pl.ds(aligned(q * size + sub * part, part), part), :]

    def w_y(m, sub):
        return remote(chunk(mats[m][0], m, dd, sub), chunk(mats[m][1], m, dd, sub),
                      w_snd.at[m, sub, 0], w_rcv.at[m, sub, 0], ynb)

    def w_x(m, sub):
        c = chunk(mats[m][1], m, dd, sub)
        return remote(c, c, w_snd.at[m, sub, 1], w_rcv.at[m, sub, 1], xnb)

    def w_c(m, sub):
        c = chunk(mats[m][1], m, dd, sub)
        return remote(c, c, w_snd.at[m, sub, 2], w_rcv.at[m, sub, 2], sib)

    def w_f(m, sub):
        c = chunk(mats[m][1], m, d_far, sub)
        return remote(c, c, w_snd.at[m, sub, 3], w_rcv.at[m, sub, 3], sib)

    def w_from(m, sub, which):
        q = (dd, d_far, d_sib, d_diag)[which]
        c = chunk(mats[m][1], m, q, sub)
        return remote(c, c, w_snd.at[m, sub, which], w_rcv.at[m, sub, which], sib)

    def got_y(m, sub):
        def fn():
            w_from(m, sub, 0).wait_recv()
            w_x(m, sub).start()
            w_c(m, sub).start()

        return fn

    def got_x(m, sub):
        def fn():
            w_from(m, sub, 1).wait_recv()
            w_f(m, sub).start()

        return fn

    def got_rest(m):
        def fn():
            for sub in range(SUBS):
                w_from(m, sub, 2).wait_recv()
                w_from(m, sub, 3).wait_recv()

        return fn

    def w_copies(kind, hf, k, pair):
        out = []
        for b in range(2):
            if kind == "u":
                src = (wu, wou)[hf].at[k, :, pl.ds(b * dim, dim)]
            else:
                src = (wd, wod)[hf].at[k, pl.ds(b * dim, dim), :]
            out.append(local(src, wb.at[2 * pair + b], s_w.at[2 * pair + b]))
        return out

    def w_load(kind, hf, k, pair):
        def fn():
            for c in w_copies(kind, hf, k, pair):
                c.start()

        return fn

    def w_wait(kind, hf, k, pair):
        def fn():
            for c in w_copies(kind, hf, k, pair):
                c.wait()

        return fn

    def run_loop(n, body, hooks):
        def f(it, carry):
            for key in sorted(hooks):
                @pl.when(it == key)
                def _(key=key):
                    for fn in hooks[key]:
                        fn()
            body(it)
            return carry

        lax.fori_loop(0, n, f, 0)

    def rslice(r):
        return pl.ds(aligned(r * bm, bm), bm)

    def zslice(r):
        return pl.ds(aligned(r * bz, bz), bz)

    def x_copy(r):
        return local(x.at[pl.ds(aligned(row0 + r * bz, bz), bz), :], res.at[zslice(r), :], s_x.at[r])

    def act_out(dst, it, half0, b, buf):
        hf = half0 + it // nz
        return local(outs.at[buf], dst.at[hf, zslice(it % nz), pl.ds(b * dim, dim)], s_out.at[buf])

    def out_waits(it, put):
        for c in put(it, 0, it):
            c.wait()

        @pl.when(it >= 1)
        def _():
            for c in put(it - 1, 1, it):
                c.wait()

    def out_starts(it, put):
        for c in put(it, 0, it):
            c.start()

        @pl.when(it >= 1)
        def _():
            for c in put(it - 1, 1, it):
                c.start()

    def z_stage(nh, half0, pair0, z_dst, a_dst, hooks, wait_x=False, ending=()):
        def epi(slot, zi, n):
            zb = gacc[slot, :bz, n].astype(BF16)
            outs[zi, :, n] = zb
            zf = zb.astype(F32)
            outs[zi + 1, :, n] = (zf * gelu_half(zf)).astype(BF16)

        def put(it, b, when):
            buf = 4 * (when % 2) + 2 * b
            return (act_out(z_dst, it, half0, b, buf), act_out(a_dst, it, half0, b, buf + 1))

        def body(it):
            r = it % nz
            base = 2 * (pair0 + it // nz)
            buf = 4 * (it % 2)
            if wait_x:
                x_copy(r).wait()

            @pl.when(it >= 2)
            def _():
                out_waits(it - 2, put)

            for n in chunks:
                gacc[0, :bz, n] = dot_nn(res[zslice(r), :], wb[base, :, n])
                epi(1, buf + 2, n)
            for n in chunks:
                gacc[1, :bz, n] = dot_nn(res[zslice(r), :], wb[base + 1, :, n])
                epi(0, buf, n)
            out_starts(it, put)

        total = nz * nh
        run_loop(total, body, hooks)
        for fn in ending:
            fn()
        out_waits(total - 2, put)
        for n in chunks:
            epi(1, 4 * (total % 2) + 2, n)
        for c in put(total - 1, 1, total):
            c.start()
        out_waits(total - 1, put)
        for c in put(total - 1, 1, total):
            c.wait()

    def k_tiles(src, hf, r):
        return [local(src.at[hf, rslice(r), pl.ds(b * dim, dim)], ring.at[(r % 2) * 2 + b], s_ring.at[(r % 2) * 2 + b])
                for b in range(2)]

    def k_first(src, hf):
        def fn():
            for c in k_tiles(src, hf, 0):
                c.start()

        return fn

    def k_stage(src, hf, pair, trans, store, hooks):
        last = store is not None

        def part(r):
            if last:
                return local(hpart.at[rslice(r), :], gacc.at[r % 2, pl.ds(0, bm), :], s_gacc.at[r % 2])
            return local(gacc.at[r % 2, pl.ds(0, bm), :], hpart.at[rslice(r), :], s_gacc.at[r % 2])

        def keep(r):
            return local(res.at[rslice(r), :], store.at[rslice(r), :], s_out.at[r % 2])

        if last:
            part(0).start()

        def body(r):
            slot = r % 2

            @pl.when(r + 1 < nr)
            def _():
                for c in k_tiles(src, hf, r + 1):
                    c.start()
                if last:
                    part(r + 1).start()

            for c in k_tiles(src, hf, r):
                c.wait()
            if last:
                part(r).wait()

                @pl.when(r >= 2)
                def _():
                    keep(r - 2).wait()
            else:
                @pl.when(r >= 2)
                def _():
                    part(r - 2).wait()
            for n in chunks:
                if trans:
                    val = dot_nt(ring[slot * 2], wb[2 * pair, n, :]) + dot_nt(ring[slot * 2 + 1], wb[2 * pair + 1, n, :])
                else:
                    val = dot_nn(ring[slot * 2], wb[2 * pair, :, n]) + dot_nn(ring[slot * 2 + 1], wb[2 * pair + 1, :, n])
                if last:
                    res[rslice(r), n] = (val + gacc[slot, :bm, n]).astype(BF16)
                else:
                    gacc[slot, :bm, n] = val
            if not last:
                part(r).start()
            else:
                keep(r).start()

        run_loop(nr, body, hooks)
        if not last:
            part(nr - 2).wait()
            part(nr - 1).wait()
        else:
            keep(nr - 2).wait()
            keep(nr - 1).wait()

    def q_tile(src, it, b):
        buf = 2 * b + it % 2
        return local(src.at[it // nz, zslice(it % nz), pl.ds(b * dim, dim)], ring.at[buf, pl.ds(0, bz), :], s_ring.at[buf])

    def q_first(src):
        def fn():
            q_tile(src, 0, 0).start()

        return fn

    def q_stage(z_src, q_dst, hooks, ending=()):
        total = 2 * nz

        def epi(slot, buf, tile, n):
            e = gacc[slot, :bz, n].astype(BF16).astype(F32)
            outs[buf, :, n] = (e * gelu_slope(ring[tile, :bz, n].astype(F32))).astype(BF16)

        def put(it, b, when):
            return (act_out(q_dst, it, 0, b, 4 * (when % 2) + 2 * b),)

        def body(it):
            r = it % nz
            base = 2 * (it // nz)
            buf = 4 * (it % 2)
            q_tile(z_src, it, 1).start()

            @pl.when(it + 1 < total)
            def _():
                q_tile(z_src, it + 1, 0).start()

            @pl.when(it >= 1)
            def _():
                q_tile(z_src, it - 1, 1).wait()

            @pl.when(it >= 2)
            def _():
                out_waits(it - 2, put)

            q_tile(z_src, it, 0).wait()
            for n in chunks:
                gacc[0, :bz, n] = dot_nt(res[zslice(r), :], wb[base, n, :])
                epi(1, buf + 2, 2 + (it + 1) % 2, n)
            for n in chunks:
                gacc[1, :bz, n] = dot_nt(res[zslice(r), :], wb[base + 1, n, :])
                epi(0, buf, it % 2, n)
            out_starts(it, put)

        run_loop(total, body, hooks)
        for fn in ending:
            fn()
        out_waits(total - 2, put)
        q_tile(z_src, total - 1, 1).wait()
        for n in chunks:
            epi(1, 4 * (total % 2) + 2, 2 + (total - 1) % 2, n)
        for c in put(total - 1, 1, total):
            c.start()
        out_waits(total - 1, put)
        for c in put(total - 1, 1, total):
            c.wait()

    alpha, beta = pl.ds(0, quart), pl.ds(quart, quart)

    def c_msg(k, t):
        slot = ORDERS[k].index(("s", t)) % 2 if t < 3 else 0
        return remote(gacc.at[slot], rc.at[k, t], g_snd.at[k, t], g_rcv.at[k, t], sib)

    def x_msg(k, i):
        src = (psm.at[k, 0, alpha], psm.at[k, 1, alpha], x3.at[k, 0])[i]
        return remote(src, rx.at[k, i], g_snd.at[k, 4 + i], g_rcv.at[k, 4 + i], xnb)

    def y_msg(k, i):
        src = (psm.at[k, 0, beta], psm.at[k, 2, beta], x3.at[k, 1])[i]
        return remote(src, ry.at[k, i], g_snd.at[k, 7 + i], g_rcv.at[k, 7 + i], ynb)

    def piece_of(s, k):
        if k == 3:
            s = s + ((s + 6) // 7) * ((8 - s) // 7) - ((s + 5) // 7) * ((9 - s) // 7)
        v = s + s // 5
        mine = (1 - v % 2) * ((v + 7) // 8)
        t = mine * (v // 2 - 1) + (1 - mine) * ((v + 1) // 2)
        oth = 1 - t % 2
        xr = 1 - t // 2
        return mine, oth, xx + xr * (1 - 2 * xx), (1 - cc) + mine * (2 * cc - 1)

    def tile_of(k, src, u, oth, xp, cp):
        krow = pl.ds(aligned((u % 2) * kr, kr), kr)
        if IS_UP[k]:
            return local(src.at[oth, krow, pl.ds(aligned(cp * dim, dim), dim)], gs.at[u % 2], s_gs.at[u % 2])
        col = pl.ds(aligned(xp * dim + cp * half, half), half)
        return local(src.at[oth, krow, col], gs.at[u % 2, :, pl.ds(0, half)], s_gs.at[u % 2])

    def g_tile(k, src, u):
        _, oth, xp, cp = piece_of(u // 2, k)
        return tile_of(k, src, u, oth, xp, cp)

    def g_first(k, src):
        def fn():
            g_tile(k, src, 0).start()

        return fn

    def g_dot(k, u, xp, n):
        krow = pl.ds(aligned((u % 2) * kr, kr), kr)
        if IS_UP[k]:
            return dot_tn(res[krow, pl.ds(aligned(xp * half, half), half)], gs[u % 2, :, n])
        return dot_tn(gs[u % 2, :, :half], res[krow, n])

    def res_copy(kind, h):
        rs = pl.ds(h * kr, kr)
        if kind in ("h", "e"):
            src = (hbuf if kind == "h" else ebuf).at[rs, :]
        else:
            src = (x if kind == "x" else dy).at[pl.ds(aligned(row0 + h * kr, kr), kr), :]
        return local(src, res.at[rs, :], s_res.at[h])

    def res_load(kind, h):
        def fn():
            res_copy(kind, h).start()

        return fn

    def g_stage(k, src, res_kind, hooks):
        pieces = ORDERS[k]
        count = len(pieces)

        def save(s):
            return local(gacc.at[s % 2], psm.at[k, pieces[s][1]], s_ps)

        def theirs(t):
            return [local(rc.at[k, t, rs], side.at[i], s_side.at[i]) for i, rs in enumerate((alpha, beta))]

        def send(t):
            if t == 0:
                x_msg(k, 0).start()
                y_msg(k, 0).start()
            elif t == 1:
                x_msg(k, 1).start()
            elif t == 2:
                y_msg(k, 1).start()

        hooks = {key: list(val) for key, val in hooks.items()}

        def first(s):
            def fn():
                if s >= 2 and pieces[s - 2][0] == "s":
                    c_msg(k, pieces[s - 2][1]).wait_send()
                if s >= 1:
                    if pieces[s - 1][0] == "s":
                        c_msg(k, pieces[s - 1][1]).start()
                    else:
                        save(s - 1).start()
                        if k == 3 and pieces[s - 1][1] == 0:
                            save(s - 1).wait()
                            send(0)
                if pieces[s][0] == "m" and not (k == 3 and s == 1):
                    c_msg(k, pieces[s][1]).wait_recv()
                    for c in theirs(pieces[s][1]):
                        c.start()

            return fn

        def second(s):
            def fn():
                if s >= 1 and pieces[s - 1][0] == "m" and not (k == 3 and pieces[s - 1][1] == 0):
                    save(s - 1).wait()
                    send(pieces[s - 1][1])
                if k == 3 and s == 1:
                    c_msg(k, pieces[s][1]).wait_recv()
                    for c in theirs(pieces[s][1]):
                        c.start()
                if pieces[s][0] == "m":
                    for c in theirs(pieces[s][1]):
                        c.wait()

            return fn

        for s in range(count):
            hooks.setdefault(2 * s, []).append(first(s))
            hooks.setdefault(2 * s + 1, []).append(second(s))
        if res_kind is not None:
            for h in range(2):
                hooks.setdefault(h, []).append(lambda h=h: res_copy(res_kind, h).wait())

        def body(u):
            @pl.when(u + 1 < 2 * count)
            def _():
                g_tile(k, src, u + 1).start()

            g_tile(k, src, u).wait()
            mine, _, xp, _ = piece_of(u // 2, k)
            again = u % 2
            slot = (u // 2) % 2
            for n in chunks:
                val = g_dot(k, u, xp, n)
                for i, rs in enumerate((slice(0, quart), slice(quart, half))):
                    more = gacc[slot, rs, n] + jnp.where(mine == 1, side[i + 2 * (1 - mine * again), :, n], 0.0)
                    gacc[slot, rs, n] = val[rs, :] + jnp.where(again == 1, more, 0.0)

        run_loop(2 * count, body, hooks)
        save(count - 1).start()
        save(count - 1).wait()
        send(pieces[count - 1][1])

    def last_tile(k, src, u):
        return tile_of(k, src, u, 0, xx, (1 - cc) + (u // 2) * (2 * cc - 1))

    def last_first(k, src, res_kind):
        def fn():
            res_load(res_kind, 0)()
            last_tile(k, src, 0).start()

        return fn

    def last_pieces(k, src, res_kind, hooks):
        res_load(res_kind, 1)()
        hooks = {key: list(val) for key, val in hooks.items()}
        for h in range(2):
            hooks.setdefault(h, []).append(lambda h=h: res_copy(res_kind, h).wait())
        hooks.setdefault(2, []).append(lambda: c_msg(k, 3).start())

        def body(u):
            @pl.when(u + 1 < 4)
            def _():
                last_tile(k, src, u + 1).start()

            last_tile(k, src, u).wait()
            slot = u // 2
            for n in chunks:
                gacc[slot, :, n] = g_dot(k, u, xx, n) + jnp.where(u % 2 == 1, gacc[slot, :, n], 0.0)

        run_loop(4, body, hooks)

    def sum_phases(k):
        def p0():
            for i in (1, 2):
                x_msg(k, i).wait_recv()
                y_msg(k, i).wait_recv()
            side_in(0, rx.at[k, 1]).start()
            side_in(1, ry.at[k, 2]).start()

        def p1():
            c_msg(k, 3).wait_send()
            c_msg(k, 3).wait_recv()
            side_in(2, rc.at[k, 3, alpha]).start()
            side_in(3, rc.at[k, 3, beta]).start()

        def p2():
            side_in(0, rx.at[k, 1]).wait()
            side_in(1, ry.at[k, 2]).wait()
            side_in(2, rc.at[k, 3, alpha]).wait()
            side_scale(0, (0, 1, 2), 0)
            side_out(0, gfin.at[k, alpha]).start()
            side_in(1, ry.at[k, 1]).start()
            side_in(2, rx.at[k, 2]).start()

        def p3():
            side_in(1, ry.at[k, 1]).wait()
            side_in(2, rx.at[k, 2]).wait()
            side_in(3, rc.at[k, 3, beta]).wait()
            side_scale(3, (1, 2, 3), quart)
            side_out(3, gfin.at[k, beta]).start()

        def p4():
            side_out(0, gfin.at[k, alpha]).wait()
            side_out(3, gfin.at[k, beta]).wait()
            if IS_UP[k]:
                to_sib(k).start()

        return p0, p1, p2, p3, p4

    nq = quart // 8

    def side_add(dst, a, b):
        side[dst] = side[a] + side[b]

    def side_scale(dst, parts, row=None):
        def f(i, acc):
            rs = pl.ds(aligned(i * 8, 8), 8)
            v = side[parts[0], rs, :]
            for p in parts[1:]:
                v = v + side[p, rs, :]
            if row is not None:
                v = v + gacc[1, pl.ds(aligned(row + i * 8, 8), 8), :]
            v = v * 0.25
            side[dst, rs, :] = v
            v = v * v
            for n in range(0, dim, 128):
                acc = acc + v[:, n:n + 128]
            return acc

        ss[...] = lax.fori_loop(0, nq, f, ss[...])

    def side_in(i, src):
        return local(src, side.at[i], s_side.at[i])

    def side_out(i, dst):
        return local(side.at[i], dst, s_side.at[i])

    def join_phases(k):
        ins = ((0, psm.at[k, 1, beta]), (1, ry.at[k, 0]), (2, psm.at[k, 2, alpha]), (3, rx.at[k, 0]))

        def pa():
            x_msg(k, 0).wait_recv()
            y_msg(k, 0).wait_recv()
            for i, s in ins:
                side_in(i, s).start()

        def pb():
            for i, s in ins:
                side_in(i, s).wait()
            side_add(0, 0, 1)
            side_add(2, 2, 3)
            side_out(0, x3.at[k, 0]).start()
            side_out(2, x3.at[k, 1]).start()

        def pc():
            side_out(0, x3.at[k, 0]).wait()
            side_out(2, x3.at[k, 1]).wait()
            x_msg(k, 2).start()
            y_msg(k, 2).start()

        return pa, pb, pc

    def to_sib(k):
        src = side.at[2 * (1 - cc)] if k == 3 else gfin.at[k, pl.ds(aligned((1 - cc) * quart, quart), quart), :]
        return remote(src, gsib.at[k // 2], f_snd.at[k // 2], f_rcv.at[k // 2], sib)

    def at(first, fns):
        return {first + i: [fn] for i, fn in enumerate(fns)}

    def merge(*tables):
        out = {}
        for table in tables:
            for key, fns in table.items():
                out.setdefault(key, []).extend(fns)
        return out

    w_load("u", 0, 0, 0)()
    for r in range(nz):
        x_copy(r).start()
    meet()
    for m in range(4):
        for sub in range(SUBS):
            w_y(m, sub).start()
    ss[...] = jnp.zeros_like(ss)

    w_wait("u", 0, 0, 0)()
    z_stage(1, 0, 0, z1, a1, merge(
        {4: [w_load("d", 0, 0, 1)]}, {9: [got_y(0, 0)]}, {15: [k_first(a1, 0)]}), wait_x=True)
    w_wait("d", 0, 0, 1)()
    k_stage(a1, 0, 1, False, None, merge(
        {1: [got_y(0, 1), got_x(0, 0)]}, {6: [got_y(1, 0), got_x(0, 1)]}, {7: [got_rest(0), w_load("u", 1, 0, 0)]}))
    w_wait("u", 1, 0, 0)()
    z_stage(1, 1, 0, z1, a1, merge(
        {3: [got_y(1, 1)]}, {6: [got_x(1, 0)]}, {9: [got_y(2, 0)]},
        {14: [got_x(1, 1)]}, {15: [k_first(a1, 1), got_rest(1), w_load("d", 1, 0, 1)]}))
    w_load("u", 0, 1, 0)()
    w_wait("d", 1, 0, 1)()
    k_stage(a1, 1, 1, False, hbuf, {3: [got_y(2, 1), got_x(2, 0)]})
    w_wait("u", 0, 1, 0)()
    z_stage(2, 0, 0, z3, a3, merge(
        {0: [got_y(3, 0), got_x(2, 1)]}, {9: [got_y(3, 1), got_x(3, 0)]},
        {11: [got_rest(2), w_load("u", 1, 1, 1)]}, {16: [w_wait("u", 1, 1, 1)]}, {20: [got_x(3, 1)]},
        {24: [res_load("dy", 0)]}, {31: [g_first(0, a3)]}), ending=(res_load("dy", 1),))
    g_stage(0, a3, "dy", merge(
        {3: [w_load("d", 0, 1, 0)]}, {5: [got_rest(3), w_load("d", 1, 1, 1)]}, {10: [q_first(z3)]}))
    w_wait("d", 0, 1, 0)()
    q_stage(z3, q3, merge(
        {16: [w_wait("d", 1, 1, 1)]}, at(8, join_phases(0)),
        {24: [res_load("h", 0)]}, {31: [g_first(1, q3)]}), ending=(res_load("h", 1),))
    g_stage(1, q3, "h", merge(
        {3: [w_load("u", 0, 1, 0)]}, {5: [w_load("u", 1, 1, 1)]}, {10: [k_first(q3, 0)]}))
    w_wait("u", 0, 1, 0)()
    k_stage(q3, 0, 0, True, None, at(5, join_phases(1)))
    k_first(q3, 1)()
    w_wait("u", 1, 1, 1)()
    k_stage(q3, 1, 1, True, ebuf, {nr - 1: [g_first(2, a1)]})
    g_stage(2, a1, None, merge(
        {3: [w_load("d", 0, 0, 0)]}, {5: [w_load("d", 1, 0, 1)]}, {10: [q_first(z1)]}))
    w_wait("d", 0, 0, 0)()
    q_stage(z1, q1, merge(
        {16: [w_wait("d", 1, 0, 1)]}, at(8, join_phases(2)),
        {24: [res_load("x", 0)]}, {31: [g_first(3, q1)]}), ending=(res_load("x", 1),))
    g_stage(3, q1, "x", {11: [last_first(0, a3, "dy")]})
    four, three, two = sum_phases(0), sum_phases(1), sum_phases(2)

    def one_in():
        x_msg(3, 1).wait_recv()
        y_msg(3, 1).wait_recv()
        side_in(0, rx.at[3, 1]).start()
        side_in(2, ry.at[3, 1]).start()

    last_pieces(0, a3, "dy", {3: [last_first(1, q3, "h")]})
    for fn in join_phases(3):
        fn()
    last_pieces(1, q3, "h", {0: [four[0], four[1]], 1: [four[2]], 2: [four[3]], 3: [four[4], last_first(2, a1, "e"), three[0]]})
    last_pieces(2, a1, "e", {0: [three[1]], 1: [three[2]], 2: [three[3]], 3: [three[4], last_first(3, q1, "x"), two[0]]})
    last_pieces(3, q1, "x", {0: [two[1]], 1: [two[2]], 2: [two[3]], 3: [two[4], one_in]})
    c_msg(3, 3).wait_send()
    c_msg(3, 3).wait_recv()
    side_in(1, rc.at[3, 3, alpha]).start()
    side_in(3, rc.at[3, 3, beta]).start()
    side_in(0, rx.at[3, 1]).wait()
    side_in(2, ry.at[3, 1]).wait()
    side_in(1, rc.at[3, 3, alpha]).wait()
    side_add(0, 0, 1)
    side_in(3, rc.at[3, 3, beta]).wait()
    side_add(2, 2, 3)
    y_msg(3, 2).wait_recv()
    side_in(1, ry.at[3, 2]).start()
    x_msg(3, 2).wait_recv()
    side_in(3, rx.at[3, 2]).start()
    side_in(1, ry.at[3, 2]).wait()
    side_scale(0, (0, 1), 0)
    side_out(0, gfin.at[3, alpha]).start()
    side_in(3, rx.at[3, 2]).wait()
    side_scale(2, (2, 3), quart)
    side_out(2, gfin.at[3, beta]).start()
    to_sib(3).start()

    nbuf[me] = ss[...]

    def n_send(o):
        tid = (me + o) % 8
        return remote(ss, nbuf.at[me], n_snd.at[o], n_rcv.at[o], (tid // 4, tid % 4))

    def n_recv(o):
        return remote(ss, nbuf.at[(me + 8 - o) % 8], n_snd.at[o], n_rcv.at[o], sib)

    for o in range(1, 8):
        n_send(o).start()
    for o in range(1, 8):
        n_recv(o).wait_recv()
    acc = nbuf[0]
    for i in range(1, 8):
        acc = acc + nbuf[i]
    nrm[...] = acc

    side_out(0, gfin.at[3, alpha]).wait()
    side_out(2, gfin.at[3, beta]).wait()
    for k in (1, 3):
        to_sib(k).wait_recv()
        to_sib(k).wait_send()
    for o in range(1, 8):
        n_send(o).wait_send()
    for m in range(4):
        for sub in range(SUBS):
            for c in (w_y(m, sub), w_x(m, sub), w_c(m, sub), w_f(m, sub)):
                c.wait_send()
    for k in range(4):
        for i in range(3):
            x_msg(k, i).wait_send()
            y_msg(k, i).wait_send()


def gradients(act_in, grad_out, w_up, w_down):
    rows = act_in.shape[0] // 2
    dim = act_in.shape[1]
    wide = w_up.shape[2]
    half, quart = dim // 2, dim // 4
    bm, bz = rows // 8, rows // 16
    hbm = pltpu.HBM
    S = jax.ShapeDtypeStruct
    act = S((2, rows, wide), BF16)
    outs = [
        S((4, half, dim), F32), S((2, quart, dim), F32), S((8, 128), F32), S((2,), jnp.int32),
        S(w_up.shape, BF16), S(w_down.shape, BF16), act, act, act, act, act, act,
        S((rows, dim), BF16), S((rows, dim), BF16), S((rows, dim), F32),
        S((4, 4, half, dim), F32), S((4, 4, half, dim), F32),
        S((4, 3, quart, dim), F32), S((4, 3, quart, dim), F32), S((4, 2, quart, dim), F32),
    ]
    out_specs = [pl.BlockSpec(memory_space=hbm) for _ in outs]
    out_specs[2] = pl.BlockSpec(memory_space=pltpu.VMEM)
    out_specs[3] = pl.BlockSpec(memory_space=pltpu.SMEM)
    dma = pltpu.SemaphoreType.DMA
    scratch = [
        pltpu.VMEM((4, dim, dim), BF16), pltpu.VMEM((4, bm, dim), BF16), pltpu.VMEM((2, half, dim), F32),
        pltpu.VMEM((8, bz, dim), BF16), pltpu.VMEM((rows, dim), BF16), pltpu.VMEM((2, rows // 2, dim), BF16),
        pltpu.VMEM((4, quart, dim), F32), pltpu.VMEM((8, 128), F32), pltpu.VMEM((8, 8, 128), F32),
        dma((16,)), dma((4,)), dma((4,)), dma((8,)), dma((2,)), dma, dma((2,)), dma((2,)), dma((4,)),
        dma((4, SUBS, 4)), dma((4, SUBS, 4)), dma((4, 10)), dma((4, 10)), dma((2,)), dma((2,)), dma((8,)), dma((8,)),
    ]
    flops = 20 * rows * dim * 2 * wide
    return pl.pallas_call(
        functools.partial(grad_kernel, rows, bm, bz, min(256, dim)),
        out_shape=outs,
        in_specs=[pl.BlockSpec(memory_space=hbm)] * 4,
        out_specs=out_specs,
        scratch_shapes=scratch,
        compiler_params=pltpu.CompilerParams(
            collective_id=0, has_side_effects=True, vmem_limit_bytes=66_900_000
        ),
        cost_estimate=pl.CostEstimate(flops=flops, bytes_accessed=1_500_000_000, transcendentals=0),
        name="grads",
    )(act_in, grad_out, w_up, w_down)[:4]


def update_kernel(is_up, where_ref, rate_ref, clip_ref, squares, *refs):
    grads, refs = refs[:1 + is_up], refs[1 + is_up:]
    master, mom, var = refs[:3]
    new_master, new_mom, new_var, wide, shard, scale = refs[-6:]
    cols = grads[0].shape[-1]

    @pl.when(pl.program_id(0) == 0)
    def _():
        norm = jnp.sqrt(jnp.sum(squares[...], keepdims=True))
        scale[...] = jnp.broadcast_to(jnp.minimum(1.0, clip_ref[0] / (norm + NORM_EPS)), scale.shape)

    clip_scale = scale[:1, :1]
    rate = rate_ref[0] / (1.0 - BETA_ONE ** STEP)
    for j in range(1 + is_up):
        cs = slice(j * cols, (j + 1) * cols)
        g = grads[0][0]
        if is_up:
            g = jnp.where(where_ref[1] == j, g, grads[1][0])
        scaled = clip_scale * g
        m = BETA_ONE * mom[0, :, cs] + (1.0 - BETA_ONE) * scaled
        v = BETA_TWO * var[0, :, cs] + ((1.0 - BETA_TWO) * scaled) * scaled
        new_mom[0, :, cs] = m
        new_var[0, :, cs] = v
        hat = v * (1.0 / (1.0 - BETA_TWO ** STEP))
        root = jnp.where(hat > 0.0, hat * lax.rsqrt(hat), 0.0)
        new = master[0, :, cs] - (rate * m) * pl.reciprocal(root + ADAM_EPS)
        new_master[0, :, cs] = new
        low = new.astype(BF16)
        wide[0, :, cs] = low
        shard[:, cs] = low


def update(is_up, k, mat, part, parts, where, scalars, gfin, gsib, state, before):
    rows, cols = state[0].shape[1:]
    blocks = next(b for b in (5, 4, 2, 1) if rows % (16 * parts * b) == 0)
    br = rows // (parts * blocks)
    skip = part * blocks
    dim = gfin.shape[2]

    def mine(i, w):
        return (mat, skip + i, 0)

    any_spec = pl.BlockSpec(memory_space=pl.ANY)
    state_spec = pl.BlockSpec((1, br, cols), mine)
    if is_up:
        g_specs = [pl.BlockSpec((1, br, dim), lambda i, w: (k, w[1] * parts * blocks + skip + i, 0)), pl.BlockSpec((1, br, dim), lambda i, w: (k // 2, skip + i, 0))]
        g_args = [gfin, gsib]
    else:
        g_specs, g_args = [pl.BlockSpec((1, br, dim), lambda i, w: (k, skip + i, 0))], [gfin]
    held = list(before) if before is not None else []
    n_in = 4 + len(g_args) + 3
    smem = pl.BlockSpec(memory_space=pltpu.SMEM)
    S = jax.ShapeDtypeStruct
    shape = state[0].shape
    return pl.pallas_call(
        functools.partial(update_kernel, int(is_up)),
        out_shape=[S(shape, F32)] * 3 + [S((2, 4 * rows, cols), BF16), S((rows // parts, cols), BF16)],
        grid_spec=pltpu.PrefetchScalarGridSpec(
            num_scalar_prefetch=1, grid=(blocks,),
            in_specs=[smem, smem, pl.BlockSpec(memory_space=pltpu.VMEM)] + g_specs + [state_spec] * 3 + [any_spec] * len(held),
            out_specs=[state_spec] * 3 + [
                pl.BlockSpec((1, br, cols), lambda i, w: (mat, w[0] * parts * blocks + skip + i, 0)), pl.BlockSpec((br, cols), lambda i, w: (i, 0))],
            scratch_shapes=[pltpu.VMEM((8, 128), F32)],
        ),
        input_output_aliases={n_in + i: i for i in range(len(held))},
        cost_estimate=pl.CostEstimate(flops=30 * rows * cols // parts, bytes_accessed=32 * rows * cols // parts, transcendentals=2 * rows * cols // parts),
        name="adam",
    )(where, *scalars, *g_args, *state, *held)


TO_FAR = [(0, 2), (2, 0), (1, 3), (3, 1)]
TO_SIB = [(0, 1), (1, 0), (2, 3), (3, 2)]


ORDER = [(up, k, mat, part, parts) for up, k, mat, parts in ((False, 2, 0, 4), (False, 0, 1, 2), (True, 3, 0, 2), (True, 1, 1, 4)) for part in range(parts)]


def solution(mesh):
    spec_rows = P("data", None)
    spec_wup = P(None, None, "model")
    spec_wdown = P(None, "model", None)
    spec_sup = P(None, "data", "model")
    spec_sdown = P(None, ("model", "data"), None)
    spec_scalar = P(None)

    def local_step(act_in, grad_out, w_up, w_down, master_up, master_down, mom_up, mom_down, var_up, var_down, learn_rate, clip_norm):
        place = lax.axis_index("data")
        core = place % 2
        side = place // 2
        gfin, gsib, squares, where = gradients(act_in, grad_out, w_up, w_down)
        norm_val = jnp.sqrt(jnp.sum(squares))
        scalars = (learn_rate, clip_norm, squares)
        state = {False: (master_down, mom_down, var_down), True: (master_up, mom_up, var_up)}
        done = {False: None, True: None}
        at_far, at_sib, at_diag = 2 * (1 - side) + core, 2 * side + 1 - core, 2 * (1 - side) + 1 - core

        def sib(shard):
            return lax.ppermute(shard, "data", TO_SIB)

        def put(is_up, mat, part, owner, piece):
            wide = done[is_up][3]
            start = owner * (wide.shape[1] // 4) + part * piece.shape[0]
            done[is_up][3] = lax.dynamic_update_slice(wide, piece[None], (mat, start, 0))

        sent = []
        for is_up, k, mat, part, parts in ORDER:
            *done[is_up], shard = update(is_up, k, mat, part, parts, where, scalars, gfin, gsib, state[is_up], done[is_up])
            where, shard = lax.optimization_barrier((where, shard))
            got = lax.ppermute(shard, "data", TO_FAR)
            sent.append((is_up, mat, part, shard, got))
        is_up, mat, part, shard, got = sent[0]
        put(is_up, mat, part, at_sib, sib(shard))
        late = None
        for i, (is_up, mat, part, shard, got) in enumerate(sent):
            got, done[True][3], done[False][3] = lax.optimization_barrier((got, done[True][3], done[False][3]))
            diag = sib(got)
            put(is_up, mat, part, at_far, got)
            if late is not None:
                put(*late)
            late = (is_up, mat, part, at_diag, diag)
            if i + 1 < len(sent):
                is_up, mat, part, shard, got = sent[i + 1]
                put(is_up, mat, part, at_sib, sib(shard))
        put(*late)
        up, down = done[True], done[False]
        new_w_up, new_w_down = up[3], down[3]
        return (new_w_up, new_w_down, up[0], down[0], up[1], down[1], up[2], down[2], norm_val.reshape(1))

    return jax.shard_map(local_step, mesh=mesh, in_specs=(spec_rows, spec_rows, spec_wup, spec_wdown, spec_sup, spec_sdown, spec_sup, spec_sdown, spec_sup, spec_sdown, spec_scalar, spec_scalar), out_specs=(spec_wup, spec_wdown, spec_sup, spec_sdown, spec_sup, spec_sdown, spec_sup, spec_sdown, spec_scalar), check_vma=False)
```
